64 devices in a mesh: req: 4 (over x, y), cp: 16 (over z, core).
Axes of the slice: x: 2, y: 2, z: 8, core: 2. Of those that a mesh axis runs over, the one named last changes fastest.
The devices are a block of a 4x4x8 slice.
Arguments:
- x: bfloat16 [16384, 2048], P(('req', 'cp')), parts along dimension 0
- token_ids: int32 [16], P('req'), parts along dimension 0
- embed_table: bfloat16 [49152, 2048], P('cp')
- norm_attn: bfloat16 [2, 2048], replicated
- w_q: bfloat16 [2, 2048, 32, 64], replicated
- w_k: bfloat16 [2, 2048, 32, 64], replicated
- w_v: bfloat16 [2, 2048, 32, 64], replicated
- w_o: bfloat16 [2, 32, 64, 2048], replicated
- norm_mlp: bfloat16 [2, 2048], replicated
- w_gate: bfloat16 [2, 2048, 8192], replicated
- w_up: bfloat16 [2, 2048, 8192], replicated
- w_down: bfloat16 [2, 8192, 2048], replicated
Outputs:
- output 1: bfloat16 [16384, 2048], P(('req', 'cp')), parts along dimension 0
- output 2: bfloat16 [2, 16384, 32, 64], P(None, 'req', 'cp'), parts along dimension 1
- output 3: bfloat16 [2, 16384, 32, 64], P(None, 'req', 'cp'), parts along dimension 1
- output 4: bfloat16 [16, 2048], P('req'), parts along dimension 0
There are 4 independent parts. The reference program is written for one: setup_inputs(seed, part) draws one part's arguments, and reference() takes and returns one part's arrays. A program takes and returns all parts, laid end to end along the dimension named above; an argument that names none is the same for every part.
All inputs are finite; a program needn't handle non-finite values.
Results may differ from the reference program's by a relative error of at most 0.0196713.
Values are sent between devices in bfloat16 or wider.
A program may use at most 768 MiB of HBM per device.

```python
import jax
import jax.numpy as jnp
from jax import lax

GROUP_SIZE = 16
SEQ_DEV = 256
NUM_LAYERS = 2
NUM_STEPS = 4
D_MODEL = 2048
NUM_HEADS = 32
KV_HEADS = 32
HEAD_DIM = 64
FF_DIM = 8192
VOCAB_SIZE = 49152
ROPE_BASE = 10000
NORM_EPS = 1e-5


def draw_normal(key, shape, scale):
    return (jax.random.normal(key, shape, jnp.float32) * scale).astype(jnp.bfloat16)


def draw_gain(key):
    return (1.0 + 0.3 * jax.random.normal(key, (NUM_LAYERS, D_MODEL), jnp.float32)).astype(jnp.bfloat16)


def setup_inputs(seed: int = 0, part: int = 0) -> dict:
    base_key = jax.random.key(seed)
    part_keys = jax.random.split(jax.random.fold_in(base_key, part), 2)
    keys = jax.random.split(base_key, 10)
    seq_len = GROUP_SIZE * SEQ_DEV
    return {
        'x': draw_normal(part_keys[0], (seq_len, D_MODEL), 1.0),
        'token_ids': jax.random.randint(part_keys[1], (NUM_STEPS,), 0, VOCAB_SIZE, dtype=jnp.int32),
        'embed_table': draw_normal(keys[0], (VOCAB_SIZE, D_MODEL), 1.0),
        'norm_attn': draw_gain(keys[1]),
        'w_q': draw_normal(keys[2], (NUM_LAYERS, D_MODEL, NUM_HEADS, HEAD_DIM), 2.0 * D_MODEL ** -0.5),
        'w_k': draw_normal(keys[3], (NUM_LAYERS, D_MODEL, KV_HEADS, HEAD_DIM), D_MODEL ** -0.5),
        'w_v': draw_normal(keys[4], (NUM_LAYERS, D_MODEL, KV_HEADS, HEAD_DIM), D_MODEL ** -0.5),
        'w_o': draw_normal(keys[5], (NUM_LAYERS, NUM_HEADS, HEAD_DIM, D_MODEL), 2.0 * (NUM_HEADS * HEAD_DIM) ** -0.5),
        'norm_mlp': draw_gain(keys[6]),
        'w_gate': draw_normal(keys[7], (NUM_LAYERS, D_MODEL, FF_DIM), D_MODEL ** -0.5),
        'w_up': draw_normal(keys[8], (NUM_LAYERS, D_MODEL, FF_DIM), D_MODEL ** -0.5),
        'w_down': draw_normal(keys[9], (NUM_LAYERS, FF_DIM, D_MODEL), FF_DIM ** -0.5),
    }


def rms_norm(rows, gain_row):
    wide_rows = rows.astype(jnp.float32)
    inv_rms = lax.rsqrt(jnp.mean(wide_rows * wide_rows, axis=-1, keepdims=True) + NORM_EPS)
    return (wide_rows * inv_rms * gain_row.astype(jnp.float32)).astype(jnp.bfloat16)


def rope_tables(positions):
    inv_freq = 1.0 / (ROPE_BASE ** (jnp.arange(0, HEAD_DIM, 2, dtype=jnp.float32) / HEAD_DIM))
    angles = positions.astype(jnp.float32)[:, None] * inv_freq[None, :]
    return jnp.cos(angles), jnp.sin(angles)


def apply_rope(vectors, cos_tab, sin_tab):
    half_dim = vectors.shape[-1] // 2
    first = vectors[..., :half_dim]
    second = vectors[..., half_dim:]
    cosines = cos_tab[..., None, :]
    sines = sin_tab[..., None, :]
    return jnp.concatenate([first * cosines - second * sines, second * cosines + first * sines], axis=-1)


def project(rows, weights):
    flat = jnp.dot(rows, weights.reshape(weights.shape[0], -1), preferred_element_type=jnp.float32)
    return flat.reshape(rows.shape[0], weights.shape[1], weights.shape[2])


def attend(queries, query_pos, keys, values, key_pos):
    num_rows = queries.shape[0]
    group_heads = NUM_HEADS // KV_HEADS
    grouped = queries.reshape(num_rows, KV_HEADS, group_heads, HEAD_DIM).astype(jnp.float32)
    scores = jnp.einsum('qhgd,khd->hgqk', grouped, keys.astype(jnp.float32)) * (HEAD_DIM ** -0.5)
    scores = jnp.where(query_pos[:, None] >= key_pos[None, :], scores, -jnp.inf)
    attn_probs = jax.nn.softmax(scores, axis=-1).astype(jnp.bfloat16)
    mixed = jnp.einsum('hgqk,khd->qhgd', attn_probs.astype(jnp.float32), values.astype(jnp.float32))
    return mixed.astype(jnp.bfloat16).reshape(num_rows, NUM_HEADS, HEAD_DIM)


def finish_layer(hidden, mixed, o_weights, gain_mlp, gate_weights, up_weights, down_weights):
    num_rows = hidden.shape[0]
    attn_out = jnp.dot(mixed.reshape(num_rows, NUM_HEADS * HEAD_DIM), o_weights.reshape(NUM_HEADS * HEAD_DIM, D_MODEL), preferred_element_type=jnp.float32)
    hidden = (hidden.astype(jnp.float32) + attn_out).astype(jnp.bfloat16)
    normed = rms_norm(hidden, gain_mlp)
    gate = jnp.dot(normed, gate_weights, preferred_element_type=jnp.float32)
    upward = jnp.dot(normed, up_weights, preferred_element_type=jnp.float32)
    gated = (jax.nn.silu(gate) * upward).astype(jnp.bfloat16)
    return (hidden.astype(jnp.float32) + jnp.dot(gated, down_weights, preferred_element_type=jnp.float32)).astype(jnp.bfloat16)


def prefill_layer(hidden, layer_weights, cos_tab, sin_tab, positions):
    gain_attn, q_weights, k_weights, v_weights, o_weights, gain_mlp, gate_weights, up_weights, down_weights = layer_weights
    seq_len = hidden.shape[0]
    normed = rms_norm(hidden, gain_attn)
    queries = apply_rope(project(normed, q_weights), cos_tab, sin_tab).astype(jnp.bfloat16)
    keys = apply_rope(project(normed, k_weights), cos_tab, sin_tab).astype(jnp.bfloat16)
    values = project(normed, v_weights).astype(jnp.bfloat16)
    block_len = SEQ_DEV // 2
    num_blocks = seq_len // block_len

    def attend_block(item):
        return attend(item[0], item[1], keys, values, positions)

    mixed = lax.map(attend_block, (queries.reshape(num_blocks, block_len, NUM_HEADS, HEAD_DIM), positions.reshape(num_blocks, block_len)))
    mixed = mixed.reshape(seq_len, NUM_HEADS, HEAD_DIM)
    hidden = finish_layer(hidden, mixed, o_weights, gain_mlp, gate_weights, up_weights, down_weights)
    return hidden, (keys, values)


def decode_layer(hidden, layer_weights, k_layer, v_layer, cos_tab, sin_tab, query_pos, key_pos):
    gain_attn, q_weights, k_weights, v_weights, o_weights, gain_mlp, gate_weights, up_weights, down_weights = layer_weights
    normed = rms_norm(hidden, gain_attn)
    queries = apply_rope(project(normed, q_weights), cos_tab, sin_tab).astype(jnp.bfloat16)
    new_keys = apply_rope(project(normed, k_weights), cos_tab, sin_tab).astype(jnp.bfloat16)
    new_values = project(normed, v_weights).astype(jnp.bfloat16)
    keys = jnp.concatenate([k_layer, new_keys], axis=0)
    values = jnp.concatenate([v_layer, new_values], axis=0)
    mixed = attend(queries, query_pos, keys, values, key_pos)
    return finish_layer(hidden, mixed, o_weights, gain_mlp, gate_weights, up_weights, down_weights)


def reference(x, token_ids, embed_table, norm_attn, w_q, w_k, w_v, w_o, norm_mlp, w_gate, w_up, w_down):
    seq_len = GROUP_SIZE * SEQ_DEV
    block_len = SEQ_DEV // 2
    stored = x.reshape(GROUP_SIZE, 2, block_len, D_MODEL)
    hidden = jnp.concatenate([stored[:, 0], stored[::-1, 1]], axis=0).reshape(seq_len, D_MODEL)
    positions = jnp.arange(seq_len, dtype=jnp.int32)
    cos_tab, sin_tab = rope_tables(positions)
    weights = (norm_attn, w_q, w_k, w_v, w_o, norm_mlp, w_gate, w_up, w_down)

    def prefill_step(carry, layer_weights):
        return prefill_layer(carry, layer_weights, cos_tab, sin_tab, positions)

    hidden, caches = lax.scan(prefill_step, hidden, weights)
    k_cache, v_cache = caches
    natural = hidden.reshape(2 * GROUP_SIZE, block_len, D_MODEL)
    x_out = jnp.stack([natural[:GROUP_SIZE], natural[GROUP_SIZE:][::-1]], axis=1).reshape(seq_len, D_MODEL)
    dec_pos = seq_len + jnp.arange(NUM_STEPS, dtype=jnp.int32)
    dec_cos, dec_sin = rope_tables(dec_pos)
    all_pos = jnp.concatenate([positions, dec_pos])

    def decode_step(carry, items):
        layer_weights, k_layer, v_layer = items
        return decode_layer(carry, layer_weights, k_layer, v_layer, dec_cos, dec_sin, dec_pos, all_pos), None

    dec_start = jnp.take(embed_table, token_ids, axis=0)
    dec_out = lax.scan(decode_step, dec_start, (weights, k_cache, v_cache))[0]
    return x_out, k_cache, v_cache, dec_out
```

```python
import functools

import jax
import jax.numpy as jnp
from jax import lax
from jax.experimental import pallas as pl
from jax.experimental.pallas import tpu as pltpu
from jax.sharding import PartitionSpec as P

ROPE_BASE = 10000.0
NORM_EPS = 1e-5
LOG2_E = 1.4426950408889634
BF16 = jnp.bfloat16
F32 = jnp.float32
MESH = pl.DeviceIdType.MESH
LANES = 128
PAD = 16
QKV_ROWS = 512
FF_TILE = 512
FF_SLOTS = 3
KEY_TILE = 512
SPLIT = 11


def pick_kernel(vocab_dev, ids_ref, base_ref, table_ref, out_ref, rows, sems):
    steps = ids_ref.shape[0]
    base = base_ref[0]

    def copy(t):
        local = jnp.clip(ids_ref[t] - base, 0, vocab_dev - 1)
        start = pl.multiple_of((local // 8) * 8, 8)
        return pltpu.make_async_copy(table_ref.at[pl.ds(start, 8), :], rows.at[t], sems.at[t])

    for t in range(steps):
        copy(t).start()
    out_ref[...] = jnp.zeros_like(out_ref)
    picked = []
    for t in range(steps):
        copy(t).wait()
        local = ids_ref[t] - base
        inside = (local >= 0) & (local < vocab_dev)
        which = jnp.where(inside, lax.rem(jnp.clip(local, 0, vocab_dev - 1), 8), -1)
        index = lax.broadcasted_iota(jnp.int32, rows.shape[1:], 0)
        picked.append(jnp.sum(jnp.where(index == which, rows[t].astype(F32), 0.0), axis=0, keepdims=True))
    picked.append(jnp.zeros((PAD - steps, rows.shape[2]), F32))
    out_ref[...] = jnp.concatenate(picked, axis=0).astype(BF16)


def pick_rows(token_ids, base, table_rows):
    vocab_dev, d_model = table_rows.shape
    steps = token_ids.shape[0]
    return pl.pallas_call(
        functools.partial(pick_kernel, vocab_dev),
        out_shape=jax.ShapeDtypeStruct((PAD, d_model), BF16),
        in_specs=[
            pl.BlockSpec(memory_space=pltpu.SMEM),
            pl.BlockSpec(memory_space=pltpu.SMEM),
            pl.BlockSpec(memory_space=pl.ANY),
        ],
        out_specs=pl.BlockSpec(memory_space=pltpu.VMEM),
        scratch_shapes=[pltpu.VMEM((steps, 8, d_model), BF16), pltpu.SemaphoreType.DMA((steps,))],
        name="pick_rows",
    )(token_ids, base, table_rows)


def main_kernel(
    group, head_dim, num_layers, steps,
    x_in, emb_in, gain_attn, gain_mlp, tables, w_q, w_k, w_v, w_o, w_gate, w_up, w_down,
    x_out, k_cache, v_cache, dec_out,
    rows_x, rows_h, mixed, sent, got, key_rows, mixed_sent, score, best, run_max, run_acc,
    qkv_ring, wo_buf, gate_ring, up_ring, down_ring, dec_w, dec_h, dec_q, dec_k, dec_v, acc, gated, emb_part, emb_full, emb_sum, dec_sent,
    sem_x, sem_qkv, sem_wo, sem_ff, sem_dec, send_qkv, recv_qkv, send_o, recv_o, send_d, recv_d, send_e, recv_e, send_f, recv_f, sem_cache, sem_out,
):
    me = lax.axis_index("cp")
    blk = LANES
    blocks = 2 * group
    d_model = rows_x.shape[1]
    ff_dim = w_gate.shape[1]
    ff_steps = ff_dim // FF_TILE
    heads_dev = LANES // head_dim
    per_tile = QKV_ROWS // LANES
    tiles = d_model // QKV_ROWS
    half = head_dim // 2
    pair_blocks = KEY_TILE // blk
    pairs = group // pair_blocks
    exp_scale = float(head_dim ** -0.5 * LOG2_E)
    acc_rows = run_acc.shape[2]
    last = num_layers - 1
    b_rows = blk + PAD
    others = group - 1
    neighbour = lax.rem(me + 1, group)
    w_qkv = (w_q, w_k, w_v)
    order_a = (1, 2, 0)

    def remote(src, dst, ssem, rsem, device):
        return pltpu.make_async_remote_copy(src_ref=src, dst_ref=dst, send_sem=ssem, recv_sem=rsem, device_id={"cp": device}, device_id_type=MESH)

    def wait_recv(ref, sem):
        remote(ref, ref, send_e, sem, neighbour).wait_recv()

    def wait_send(ref, sem):
        remote(ref, ref, sem, recv_e, neighbour).wait_send()

    def tile_of(r):
        return lax.rem(r + me // per_tile + 1, tiles)

    def qkv_copy(layer, tensor, r):
        start = pl.multiple_of(layer * d_model + tile_of(r) * QKV_ROWS, QKV_ROWS)
        return pltpu.make_async_copy(w_qkv[tensor].at[pl.ds(start, QKV_ROWS), :], qkv_ring.at[r], sem_qkv.at[r])

    def wo_copy(layer, n):
        start = pl.multiple_of(layer * d_model, d_model)
        return pltpu.make_async_copy(w_o.at[pl.ds(start, d_model), pl.ds(n * QKV_ROWS, QKV_ROWS)], wo_buf.at[n], sem_wo.at[n])

    def gu_copies(layer, step):
        slot = lax.rem(step, FF_SLOTS)
        start = pl.multiple_of(layer * d_model, d_model)
        col = pl.multiple_of(step * FF_TILE, FF_TILE)
        return (
            pltpu.make_async_copy(w_gate.at[pl.ds(start, d_model), pl.ds(col, FF_TILE)], gate_ring.at[slot], sem_ff.at[0, slot]),
            pltpu.make_async_copy(w_up.at[pl.ds(start, d_model), pl.ds(col, FF_TILE)], up_ring.at[slot], sem_ff.at[1, slot]),
        )

    def down_copy(layer, step):
        slot = lax.rem(step, FF_SLOTS)
        start = pl.multiple_of(layer * ff_dim + step * FF_TILE, FF_TILE)
        return pltpu.make_async_copy(w_down.at[pl.ds(start, FF_TILE), :], down_ring.at[slot], sem_ff.at[2, slot])

    def dec_copy(layer, tensor):
        start = pl.multiple_of(layer * d_model + me * LANES, LANES)
        return pltpu.make_async_copy(w_qkv[tensor].at[pl.ds(start, LANES), :], dec_w.at[tensor], sem_dec.at[tensor])

    def block_of(chunk, device):
        return device if chunk == 0 else blocks - 1 - device

    def qkv_piece(layer, tensor, chunk, device):
        return remote(
            sent.at[tensor, chunk, device], got.at[layer, tensor, block_of(chunk, me)],
            send_qkv.at[chunk, tensor], recv_qkv.at[layer, chunk, tensor], device,
        )

    def send_to(piece, device):
        @pl.when(device != me)
        def _():
            piece.start()

    def send_all(layer, tensor, chunk):
        def body(i, carry):
            device = lax.rem(me + 1 + i, group)
            qkv_piece(layer, tensor, chunk, device).start()
            return carry

        lax.fori_loop(0, others, body, 0)

    def normalize(read, row0, count, gain):
        part = 64 if count % 64 == 0 else 48

        def body(i, carry):
            rows = pl.ds(pl.multiple_of(i * part, 16), part)
            wide = read(rows)
            inv = lax.rsqrt(jnp.mean(wide * wide, axis=-1, keepdims=True) + NORM_EPS)
            rows_h[pl.ds(pl.multiple_of(row0 + i * part, 16), part), :] = (wide * inv * gain).astype(BF16)
            return carry

        lax.fori_loop(0, count // part, body, 0)

    def normalize_x(row0, count, gain):
        def read(rows):
            return rows_x[pl.ds(pl.multiple_of(row0 + rows.start, 16), rows.size), :].astype(F32)

        normalize(read, row0, count, gain)

    def rotate(flat, which):
        cosines, sines = tables[2 * which], tables[2 * which + 1]
        heads = flat.reshape(flat.shape[0] // head_dim, head_dim, flat.shape[1])
        first, second = heads[:, :half], heads[:, half:]
        turned = jnp.concatenate([first * cosines - second * sines, second * cosines + first * sines], axis=1)
        return turned.reshape(flat.shape)

    def project(layer, chunk):
        order = order_a if chunk == 0 else order_a[::-1]
        for place, tensor in enumerate(order):
            def body(r, carry, place=place, tensor=tensor):
                if chunk == 0 or place > 0:
                    qkv_copy(layer, tensor, r).wait()
                flat = lax.dot_general(
                    qkv_ring[r], rows_h[chunk * blk:(chunk + 1) * blk, :], (((1,), (1,)), ((), ())), preferred_element_type=F32
                )
                if tensor != 2:
                    flat = rotate(flat, chunk)
                first = tile_of(r) * per_tile
                sent[tensor, chunk, pl.ds(first, per_tile)] = flat.astype(BF16).reshape(per_tile, LANES, blk)
                if chunk == 0 or tensor == 0:
                    for i in range(per_tile):
                        send_to(qkv_piece(layer, tensor, chunk, first + i), first + i)
                if place < 2:
                    qkv_copy(layer, order[place + 1], r).start()
                elif chunk == 1:
                    @pl.when(layer < last)
                    def _():
                        qkv_copy(layer + 1, order_a[0], r).start()
                return carry

            lax.fori_loop(0, tiles, body, 0)
            got[layer, tensor, block_of(chunk, me)] = sent[tensor, chunk, me]

    def project_decode(layer):
        dec_h[0:PAD] = rows_h[2 * blk:2 * blk + PAD]
        dec_h[head_dim:head_dim + PAD] = rows_h[2 * blk:2 * blk + PAD]
        for tensor in range(3):
            dec_copy(layer, tensor).wait()
            flat = lax.dot_general(dec_w[tensor], dec_h[...], (((1,), (1,)), ((), ())), preferred_element_type=F32)
            if tensor != 2:
                flat = rotate(flat, 2)
            if tensor == 0:
                row = lax.broadcasted_iota(jnp.int32, flat.shape, 0) // head_dim
                col = lax.broadcasted_iota(jnp.int32, flat.shape, 1) // head_dim
                dec_q[...] = jnp.where(row == col, flat, 0.0).astype(BF16)
            elif tensor == 1:
                dec_k[...] = flat.T.astype(BF16)
            else:
                dec_v[...] = flat.astype(BF16)

        @pl.when(layer < last)
        def _():
            for tensor in range(3):
                dec_copy(layer + 1, tensor).start()

    def turn_keys(layer, chunk):
        def body(i, carry):
            for u in range(4):
                j = chunk * group + 4 * i + u
                key_rows[pl.ds(pl.multiple_of(j * blk, blk), blk), :] = got[layer, 1, j].astype(F32).T.astype(BF16)
            return carry

        lax.fori_loop(0, group // 4, body, 0)

    def save_cache(layer, chunk):
        def body(i, carry):
            j = chunk * group + i
            place = pl.ds(pl.multiple_of(j * blk, blk), blk)
            pltpu.make_async_copy(got.at[layer, 1, j], k_cache.at[layer, :, place], sem_cache.at[layer, 0]).start()
            pltpu.make_async_copy(got.at[layer, 2, j], v_cache.at[layer, :, place], sem_cache.at[layer, 1]).start()
            return carry

        lax.fori_loop(0, group, body, 0)

    def scores(layer, pair, tile, slot):
        keys = key_rows[pl.ds(pl.multiple_of(tile * KEY_TILE, KEY_TILE), KEY_TILE), :]
        for u in range(2):
            query = jnp.concatenate([got[layer, 0, pair_blocks * pair + 2 * u], got[layer, 0, pair_blocks * pair + 2 * u + 1]], axis=1)
            blank = jnp.zeros((head_dim, query.shape[1]), BF16)
            for h in range(heads_dev):
                parts = [blank] * heads_dev
                parts[h] = query[h * head_dim:(h + 1) * head_dim]
                value = jnp.dot(keys, jnp.concatenate(parts, axis=0), preferred_element_type=F32)
                score[slot, 2 * u + h] = value
                best[slot, 2 * u + h] = jnp.max(value, axis=0, keepdims=True)

    def absorb(layer, tile, slot, place):
        held = [got[layer, 2, tile * pair_blocks + i] for i in range(pair_blocks)]
        ones = jnp.ones((acc_rows - head_dim, KEY_TILE), BF16)
        for u in range(2):
            for h in range(heads_dev):
                c = 2 * u + h
                old = run_max[place, c]
                new = jnp.maximum(old, best[slot, c])
                probs = jnp.exp2((score[slot, c] - new) * exp_scale).astype(BF16)
                shrink = jnp.exp2((old - new) * exp_scale)
                value = jnp.concatenate([jnp.concatenate([b[h * head_dim:(h + 1) * head_dim] for b in held], axis=1), ones], axis=0)
                run_max[place, c] = new
                run_acc[place, c] = run_acc[place, c] * shrink + jnp.dot(value, probs, preferred_element_type=F32)

    def mask_diagonal(slot):
        key = lax.broadcasted_iota(jnp.int32, score.shape[2:], 0)
        query = lax.broadcasted_iota(jnp.int32, score.shape[2:], 1)
        for u in range(2):
            for h in range(heads_dev):
                value = jnp.where(key <= query + u * score.shape[3], score[slot, 2 * u + h], -jnp.inf)
                score[slot, 2 * u + h] = value
                best[slot, 2 * u + h] = jnp.max(value, axis=0, keepdims=True)

    def fresh_state(place):
        run_max[place] = jnp.full(run_max.shape[1:], -jnp.inf, F32)
        run_acc[place] = jnp.zeros(run_acc.shape[1:], F32)

    def hand_out(layer, chunk, pair, place):
        for u in range(2):
            full = jnp.concatenate(
                [run_acc[place, 2 * u + h, :head_dim] / run_acc[place, 2 * u + h, head_dim:head_dim + 1] for h in range(heads_dev)], axis=0
            )
            turned = full.T.astype(BF16)
            for i in range(2):
                j = pair_blocks * pair + 2 * u + i
                mixed_sent[j] = turned[i * blk:(i + 1) * blk]
                device = j if chunk == 0 else blocks - 1 - j
                where = mixed.at[layer, chunk * blk:(chunk + 1) * blk, pl.ds(pl.multiple_of(me * LANES, LANES), LANES)]
                send_to(remote(mixed_sent.at[j], where, send_o.at[chunk], recv_o.at[layer, chunk], device), device)

                @pl.when(device == me)
                def _(j=j):
                    mixed[layer, chunk * blk:(chunk + 1) * blk, pl.ds(pl.multiple_of(me * LANES, LANES), LANES)] = mixed_sent[j]

    def triangle(s):
        j = sum((s >= (k * (k + 1)) // 2).astype(jnp.int32) for k in range(1, pairs))
        return j, s - (j * (j + 1)) // 2

    def attend_triangle(layer, chunk):
        base = chunk * pairs
        count = pairs * (pairs + 1) // 2

        def one(s, slot):
            pair, tile = triangle(s)
            after, after_tile = triangle(jnp.minimum(s + 1, count - 1))
            if chunk == 0:
                @pl.when(tile == 0)
                def _():
                    fresh_state(pair)

            @pl.when(tile == pair)
            def _():
                mask_diagonal(slot)

            scores(layer, base + after, base + after_tile, 1 - slot)
            absorb(layer, base + tile, slot, pair)

            @pl.when(tile == pair)
            def _():
                hand_out(layer, chunk, base + pair, pair)

        scores(layer, base, base, 0)

        def body(i, carry):
            one(2 * i, 0)
            one(2 * i + 1, 1)
            return carry

        lax.fori_loop(0, count // 2, body, 0)

    def attend_square(layer):
        count = pairs * pairs

        def one(s, slot):
            pair, tile = s // pairs, lax.rem(s, pairs)
            after = jnp.minimum(s + 1, count - 1)

            @pl.when(tile == 0)
            def _():
                fresh_state(pair)

            scores(layer, pairs + after // pairs, lax.rem(after, pairs), 1 - slot)
            absorb(layer, tile, slot, pair)

        scores(layer, pairs, 0, 0)

        def body(i, carry):
            one(2 * i, 0)
            one(2 * i + 1, 1)
            return carry

        lax.fori_loop(0, count // 2, body, 0)

    def attend_decode(layer):
        ones = jnp.ones((PAD, KEY_TILE), BF16)
        queries = dec_q[...]

        def step(value_rows, value, carry):
            old, total = carry
            new = jnp.maximum(old, jnp.max(value, axis=0, keepdims=True))
            probs = jnp.exp2((value - new) * exp_scale).astype(BF16)
            shrink = jnp.exp2((old - new) * exp_scale)
            return new, total * shrink + jnp.dot(value_rows, probs, preferred_element_type=F32)

        def body(tile, carry):
            keys = key_rows[pl.ds(pl.multiple_of(tile * KEY_TILE, KEY_TILE), KEY_TILE), :]
            value = jnp.dot(keys, queries, preferred_element_type=F32)
            held = jnp.concatenate([got[layer, 2, tile * pair_blocks + i] for i in range(pair_blocks)], axis=1)
            return step(jnp.concatenate([held, ones], axis=0), value, carry)

        state = (jnp.full((1, LANES), -jnp.inf, F32), jnp.zeros((LANES + PAD, LANES), F32))
        state = lax.fori_loop(0, blocks // pair_blocks, body, state)
        value = jnp.dot(dec_k[...], queries, preferred_element_type=F32)
        key = lax.broadcasted_iota(jnp.int32, value.shape, 0)
        query = lax.rem(lax.broadcasted_iota(jnp.int32, value.shape, 1), head_dim)
        value = jnp.where((key <= query) & (key < steps), value, -jnp.inf)
        held = jnp.concatenate([dec_v[...], ones[:, :LANES]], axis=0)
        _, total = step(held, value, state)
        turned = (total[:LANES] / total[LANES:LANES + 1]).T
        lane = lax.broadcasted_iota(jnp.int32, (PAD, LANES), 1)
        result = turned[0:PAD]
        for h in range(1, heads_dev):
            result = jnp.where(lane >= h * head_dim, turned[h * head_dim:h * head_dim + PAD], result)
        dec_sent[...] = result.astype(BF16)
        mine = pl.ds(pl.multiple_of(me * LANES, LANES), LANES)
        mixed[layer, 2 * blk:2 * blk + PAD, mine] = dec_sent[...]

        def send(i, carry):
            device = lax.rem(me + 1 + i, group)
            remote(dec_sent, mixed.at[layer, 2 * blk:2 * blk + PAD, mine], send_d, recv_d.at[layer], device).start()
            return carry

        lax.fori_loop(0, others, send, 0)

    def dense(layer, chunk, between):
        row0, count = (0, blk) if chunk == 0 else (blk, b_rows)
        rows = slice(row0, row0 + count)
        for n in range(tiles):
            if chunk == 0:
                wo_copy(layer, n).wait()
            cols = slice(n * QKV_ROWS, (n + 1) * QKV_ROWS)
            added = rows_x[rows, cols].astype(F32) + jnp.dot(mixed[layer, rows, :], wo_buf[n], preferred_element_type=F32)
            acc[:count, cols] = added.astype(BF16).astype(F32)
        if chunk == 1:
            @pl.when(layer < last)
            def _():
                for n in range(tiles):
                    wo_copy(layer + 1, n).start()

        normalize(lambda r: acc[r, :], row0, count, gain_mlp[layer])

        def step_at(k):
            return k if chunk == 0 else ff_steps - 1 - k

        def widen(k):
            step = step_at(k)
            slot = lax.rem(step, FF_SLOTS)

            def ready():
                for copy in gu_copies(layer, step):
                    copy.wait()

            if chunk == 0:
                ready()
            else:
                pl.when(k >= FF_SLOTS)(ready)
            normed = rows_h[rows, :]
            gate = jnp.dot(normed, gate_ring[slot], preferred_element_type=F32)
            upward = jnp.dot(normed, up_ring[slot], preferred_element_type=F32)
            gated[:count] = (jax.nn.silu(gate) * upward).astype(BF16)

        def narrow(k):
            step = step_at(k)
            slot = lax.rem(step, FF_SLOTS)

            def ready():
                down_copy(layer, step).wait()

            if chunk == 0:
                ready()
            else:
                pl.when(k >= FF_SLOTS)(ready)
            acc[:count] += jnp.dot(gated[:count], down_ring[slot], preferred_element_type=F32)

        def refill(k, start):
            if chunk == 0:
                @pl.when(k + FF_SLOTS < ff_steps)
                def _():
                    start(layer, k + FF_SLOTS)
            else:
                step = step_at(k)

                @pl.when(step >= FF_SLOTS)
                def _():
                    start(layer, step - FF_SLOTS)

                @pl.when((step < FF_SLOTS) & (layer < last))
                def _():
                    start(layer + 1, step)

        def start_gu(which, step):
            for copy in gu_copies(which, step):
                copy.start()

        def start_down(which, step):
            down_copy(which, step).start()

        widen(0)
        refill(0, start_gu)

        def body(k, carry):
            narrow(k - 1)
            widen(k)
            refill(k - 1, start_down)
            refill(k, start_gu)
            return carry

        if between is None:
            lax.fori_loop(1, ff_steps, body, 0)
        else:
            lax.fori_loop(1, SPLIT, body, 0)
            between()
            lax.fori_loop(SPLIT, ff_steps, body, 0)
        narrow(ff_steps - 1)
        refill(ff_steps - 1, start_down)
        rows_x[rows, :] = acc[:count].astype(BF16)

    pltpu.make_async_copy(x_in, rows_x.at[0:2 * blk], sem_x).start()
    for r in range(tiles):
        qkv_copy(0, order_a[0], r).start()
    for tensor in range(3):
        dec_copy(0, tensor).start()
    for n in range(tiles):
        wo_copy(0, n).start()
    for step in range(FF_SLOTS):
        for copy in gu_copies(0, step):
            copy.start()
        down_copy(0, step).start()

    barrier = pltpu.get_barrier_semaphore()
    for i in range(1, group):
        pl.semaphore_signal(barrier, inc=1, device_id={"cp": lax.rem(me + i, group)}, device_id_type=MESH)
    dec_h[...] = jnp.zeros_like(dec_h)
    pltpu.make_async_copy(x_in, rows_x.at[0:2 * blk], sem_x).wait()
    normalize_x(0, 2 * blk, gain_attn[0])
    pl.semaphore_wait(barrier, others)

    my_cols = pl.ds(pl.multiple_of(me * LANES, LANES), LANES)

    def part_out(i, carry):
        device = lax.rem(me + 1 + i, group)
        cols = pl.ds(pl.multiple_of(device * LANES, LANES), LANES)
        remote(emb_in.at[:, cols], emb_part.at[me], send_e, recv_e, device).start()
        return carry

    lax.fori_loop(0, others, part_out, 0)
    emb_part[me] = emb_in[:, my_cols]
    project(0, 0)
    wait_recv(emb_part.at[0:others], recv_e)
    emb_sum[...] = jnp.sum(emb_part[...].astype(F32), axis=0).astype(BF16)
    emb_full[:, my_cols] = emb_sum[...]

    def sum_out(i, carry):
        device = lax.rem(me + 1 + i, group)
        remote(emb_sum, emb_full.at[:, my_cols], send_f, recv_f, device).start()
        return carry

    lax.fori_loop(0, others, sum_out, 0)

    def layer_body(layer, carry):
        project(layer, 1)

        @pl.when(layer == 0)
        def _():
            wait_recv(emb_part.at[0:others], recv_f)
            rows_x[2 * blk:2 * blk + PAD] = emb_full[...]
            wide = emb_full[...].astype(F32)
            inv = lax.rsqrt(jnp.mean(wide * wide, axis=-1, keepdims=True) + NORM_EPS)
            rows_h[2 * blk:2 * blk + PAD] = (wide * inv * gain_attn[0]).astype(BF16)

        project_decode(layer)
        for tensor in range(3):
            wait_recv(got.at[layer, tensor, 0:others], recv_qkv.at[layer, 0, tensor])
        turn_keys(layer, 0)
        save_cache(layer, 0)
        attend_triangle(layer, 0)
        send_all(layer, 1, 1)
        send_all(layer, 2, 1)
        wait_recv(got.at[layer, 0, 0:others], recv_qkv.at[layer, 1, 0])
        attend_square(layer)
        for tensor in range(3):
            wait_send(sent.at[tensor, 0, 0:others], send_qkv.at[0, tensor])
        wait_recv(mixed_sent.at[0:others], recv_o.at[layer, 0])

        def finish_attention():
            for tensor in (1, 2):
                wait_recv(got.at[layer, tensor, 0:others], recv_qkv.at[layer, 1, tensor])
            turn_keys(layer, 1)
            attend_triangle(layer, 1)
            attend_decode(layer)
            save_cache(layer, 1)

        dense(layer, 0, finish_attention)
        for tensor in range(3):
            wait_send(sent.at[tensor, 1, 0:others], send_qkv.at[1, tensor])
        wait_send(mixed_sent.at[0:others], send_o.at[0])

        @pl.when(layer < last)
        def _():
            normalize_x(0, blk, gain_attn[layer + 1])
            project(layer + 1, 0)

        @pl.when(layer == last)
        def _():
            pltpu.make_async_copy(rows_x.at[0:blk], x_out.at[0:blk], sem_out.at[0]).start()

        wait_recv(mixed_sent.at[0:others], recv_o.at[layer, 1])
        wait_recv(emb_part.at[0:others], recv_d.at[layer])
        dense(layer, 1, None)
        wait_send(mixed_sent.at[0:others], send_o.at[1])
        wait_send(emb_part.at[0:others], send_d)

        @pl.when(layer < last)
        def _():
            normalize_x(blk, b_rows, gain_attn[layer + 1])

        return carry

    lax.fori_loop(0, num_layers, layer_body, 0)

    pltpu.make_async_copy(rows_x.at[blk:2 * blk], x_out.at[blk:2 * blk], sem_out.at[1]).start()
    dec_out[...] = rows_x[2 * blk:2 * blk + PAD]
    wait_send(emb_part.at[0:others], send_e)
    wait_send(emb_part.at[0:others], send_f)
    for layer in range(num_layers):
        pltpu.make_async_copy(k_cache.at[layer], k_cache.at[layer], sem_cache.at[layer, 0]).wait()
        pltpu.make_async_copy(v_cache.at[layer], v_cache.at[layer], sem_cache.at[layer, 1]).wait()
    for part in range(2):
        where = pl.ds(part * blk, blk)
        pltpu.make_async_copy(rows_x.at[where], x_out.at[where], sem_out.at[part]).wait()


def solution(mesh):
    group = mesh.shape["cp"]

    def local_program(x_rows, token_ids, table_rows, norm_attn, w_q, w_k, w_v, w_o, norm_mlp, w_gate, w_up, w_down):
        device = lax.axis_index("cp")
        num_layers, d_model, num_heads, head_dim = w_q.shape
        kv_heads = w_k.shape[2]
        ff_dim = w_gate.shape[2]
        seq_dev = x_rows.shape[0]
        blk = seq_dev // 2
        seq_len = group * seq_dev
        steps = token_ids.shape[0]
        heads_dev = num_heads // group
        assert heads_dev * head_dim == LANES and kv_heads == num_heads and blk == LANES

        emb = pick_rows(token_ids, (device * table_rows.shape[0]).reshape(1), table_rows)

        offsets = jnp.arange(LANES, dtype=jnp.int32)
        positions = jnp.stack([device * blk + offsets, (2 * group - 1 - device) * blk + offsets, seq_len + offsets % head_dim])
        inv_freq = 1.0 / (ROPE_BASE ** (jnp.arange(0, head_dim, 2, dtype=F32) / head_dim))
        angles = positions.astype(F32)[:, None, :] * inv_freq[None, :, None]
        tables = jnp.stack([jnp.cos(angles), jnp.sin(angles)], axis=1).reshape(6, head_dim // 2, LANES)

        def head_rows(w):
            return w.transpose(0, 2, 3, 1).reshape(num_layers * num_heads * head_dim, d_model)

        any_spec = pl.BlockSpec(memory_space=pl.ANY)
        vmem = pl.BlockSpec(memory_space=pltpu.VMEM)
        dma = pltpu.SemaphoreType.DMA
        acc_rows = head_dim + 8
        quarter = KEY_TILE // 2
        tiles = d_model // QKV_ROWS
        pairs = group * blk // KEY_TILE
        scratch = [
            pltpu.VMEM((2 * blk + PAD, d_model), BF16),
            pltpu.VMEM((2 * blk + PAD, d_model), BF16),
            pltpu.VMEM((num_layers, 2 * blk + PAD, d_model), BF16),
            pltpu.VMEM((3, 2, group, LANES, blk), BF16),
            pltpu.VMEM((num_layers, 3, 2 * group, LANES, blk), BF16),
            pltpu.VMEM((seq_len, LANES), BF16),
            pltpu.VMEM((2 * group, blk, LANES), BF16),
            pltpu.VMEM((2, 2 * heads_dev, KEY_TILE, quarter), F32),
            pltpu.VMEM((2, 2 * heads_dev, 1, quarter), F32),
            pltpu.VMEM((pairs, 2 * heads_dev, 1, quarter), F32),
            pltpu.VMEM((pairs, 2 * heads_dev, acc_rows, quarter), F32),
            pltpu.VMEM((tiles, QKV_ROWS, d_model), BF16),
            pltpu.VMEM((tiles, d_model, QKV_ROWS), BF16),
            pltpu.VMEM((FF_SLOTS, d_model, FF_TILE), BF16),
            pltpu.VMEM((FF_SLOTS, d_model, FF_TILE), BF16),
            pltpu.VMEM((FF_SLOTS, FF_TILE, d_model), BF16),
            pltpu.VMEM((3, LANES, d_model), BF16),
            pltpu.VMEM((LANES, d_model), BF16),
            pltpu.VMEM((LANES, LANES), BF16),
            pltpu.VMEM((LANES, LANES), BF16),
            pltpu.VMEM((LANES, LANES), BF16),
            pltpu.VMEM((blk + PAD, d_model), F32),
            pltpu.VMEM((blk + PAD, FF_TILE), BF16),
            pltpu.VMEM((group, PAD, LANES), BF16),
            pltpu.VMEM((PAD, d_model), BF16),
            pltpu.VMEM((PAD, LANES), BF16),
            pltpu.VMEM((PAD, LANES), BF16),
            dma, dma((tiles,)), dma((tiles,)), dma((3, FF_SLOTS)), dma((3,)),
            dma((2, 3)), dma((num_layers, 2, 3)), dma((2,)), dma((num_layers, 2)), dma, dma((num_layers,)),
            dma, dma, dma, dma, dma((num_layers, 2)), dma((2,)),
        ]
        x_new, k_flat, v_flat, dec = pl.pallas_call(
            functools.partial(main_kernel, group, head_dim, num_layers, steps),
            out_shape=(
                jax.ShapeDtypeStruct((seq_dev, d_model), BF16),
                jax.ShapeDtypeStruct((num_layers, LANES, seq_len), BF16),
                jax.ShapeDtypeStruct((num_layers, LANES, seq_len), BF16),
                jax.ShapeDtypeStruct((PAD, d_model), BF16),
            ),
            in_specs=[any_spec, vmem, vmem, vmem, vmem] + [any_spec] * 7,
            out_specs=(any_spec, any_spec, any_spec, vmem),
            scratch_shapes=scratch,
            compiler_params=pltpu.CompilerParams(collective_id=0, has_side_effects=True, vmem_limit_bytes=66_000_000),
            name="prefill_decode",
        )(
            x_rows, emb, norm_attn.astype(F32)[:, None, :], norm_mlp.astype(F32)[:, None, :], tables,
            head_rows(w_q), head_rows(w_k), head_rows(w_v), w_o.reshape(num_layers * d_model, d_model),
            w_gate.reshape(num_layers * d_model, ff_dim), w_up.reshape(num_layers * d_model, ff_dim), w_down.reshape(num_layers * ff_dim, d_model),
        )

        def cache(flat):
            return flat.reshape(num_layers, heads_dev, head_dim, seq_len).transpose(0, 3, 1, 2)

        return x_new, cache(k_flat), cache(v_flat), dec[:steps]

    replicated = P()
    in_specs = (P(("req", "cp"), None), P("req"), P("cp", None)) + (replicated,) * 9
    out_specs = (P(("req", "cp"), None), P(None, "req", "cp", None), P(None, "req", "cp", None), P("req", None))
    return jax.shard_map(local_program, mesh=mesh, in_specs=in_specs, out_specs=out_specs, check_vma=False)
```

```python
import functools

import jax
import jax.numpy as jnp
from jax import lax
from jax.experimental import pallas as pl
from jax.experimental.pallas import tpu as pltpu
from jax.sharding import PartitionSpec as P

ROPE_BASE = 10000.0
NORM_EPS = 1e-5
LOG2_E = 1.4426950408889634
BF16 = jnp.bfloat16
F32 = jnp.float32
MESH = pl.DeviceIdType.MESH
LANES = 128
PAD = 16
QKV_ROWS = 512
FF_TILE = 512
FF_SLOTS = 4
KEY_TILE = 512
SPLIT = (14, 12)


def pick_kernel(vocab_dev, ids_ref, base_ref, table_ref, out_ref, rows, sems):
    steps = ids_ref.shape[0]
    base = base_ref[0]

    def copy(t):
        local = jnp.clip(ids_ref[t] - base, 0, vocab_dev - 1)
        start = pl.multiple_of((local // 8) * 8, 8)
        return pltpu.make_async_copy(table_ref.at[pl.ds(start, 8), :], rows.at[t], sems.at[t])

    for t in range(steps):
        copy(t).start()
    out_ref[...] = jnp.zeros_like(out_ref)
    picked = []
    for t in range(steps):
        copy(t).wait()
        local = ids_ref[t] - base
        inside = (local >= 0) & (local < vocab_dev)
        which = jnp.where(inside, lax.rem(jnp.clip(local, 0, vocab_dev - 1), 8), -1)
        index = lax.broadcasted_iota(jnp.int32, rows.shape[1:], 0)
        picked.append(jnp.sum(jnp.where(index == which, rows[t].astype(F32), 0.0), axis=0, keepdims=True))
    picked.append(jnp.zeros((PAD - steps, rows.shape[2]), F32))
    out_ref[...] = jnp.concatenate(picked, axis=0).astype(BF16)


def pick_rows(token_ids, base, table_rows):
    vocab_dev, d_model = table_rows.shape
    steps = token_ids.shape[0]
    return pl.pallas_call(
        functools.partial(pick_kernel, vocab_dev),
        out_shape=jax.ShapeDtypeStruct((PAD, d_model), BF16),
        in_specs=[
            pl.BlockSpec(memory_space=pltpu.SMEM),
            pl.BlockSpec(memory_space=pltpu.SMEM),
            pl.BlockSpec(memory_space=pl.ANY),
        ],
        out_specs=pl.BlockSpec(memory_space=pltpu.VMEM),
        scratch_shapes=[pltpu.VMEM((steps, 8, d_model), BF16), pltpu.SemaphoreType.DMA((steps,))],
        name="pick_rows",
    )(token_ids, base, table_rows)


def main_kernel(
    group, head_dim, num_layers, steps,
    x_in, emb_in, gain_attn, gain_mlp, tables, w_q, w_k, w_v, w_o, w_gate, w_up, w_down,
    x_out, k_cache, v_cache, dec_out,
    rows_x, rows_h, mixed, sent, got_q, got, key_rows, mixed_sent, score, best, run_max, run_acc,
    qkv_ring, wo_buf, gate_ring, up_ring, down_ring, dec_w, dec_h, dec_q, dec_k, dec_v, acc, gated, emb_part, emb_full, emb_sum, dec_sent,
    sem_x, sem_qkv, sem_wo, sem_ff, sem_dec, send_qkv, recv_qkv, send_o, recv_o, send_d, recv_d, send_e, recv_e, send_f, recv_f, sem_cache, sem_out,
):
    me = lax.axis_index("cp")
    blk = LANES
    blocks = 2 * group
    d_model = rows_x.shape[1]
    ff_dim = w_gate.shape[1]
    ff_steps = ff_dim // FF_TILE
    heads_dev = LANES // head_dim
    per_tile = QKV_ROWS // LANES
    tiles = d_model // QKV_ROWS
    half = head_dim // 2
    pair_blocks = KEY_TILE // blk
    pairs = group // pair_blocks
    exp_scale = float(head_dim ** -0.5 * LOG2_E)
    acc_rows = run_acc.shape[2]
    last = num_layers - 1
    b_rows = blk + PAD
    others = group - 1
    neighbour = lax.rem(me + 1, group)
    w_qkv = (w_q, w_k, w_v)
    order_a = (1, 2, 0)

    def remote(src, dst, ssem, rsem, device):
        return pltpu.make_async_remote_copy(src_ref=src, dst_ref=dst, send_sem=ssem, recv_sem=rsem, device_id={"cp": device}, device_id_type=MESH)

    def wait_recv(ref, sem):
        remote(ref, ref, send_e, sem, neighbour).wait_recv()

    def wait_send(ref, sem):
        remote(ref, ref, sem, recv_e, neighbour).wait_send()

    def tile_of(r):
        return lax.rem(r + me // per_tile + 1, tiles)

    def qkv_copy(layer, tensor, r):
        start = pl.multiple_of(layer * d_model + tile_of(r) * QKV_ROWS, QKV_ROWS)
        return pltpu.make_async_copy(w_qkv[tensor].at[pl.ds(start, QKV_ROWS), :], qkv_ring.at[r], sem_qkv.at[r])

    def wo_copy(layer, n):
        start = pl.multiple_of(layer * d_model, d_model)
        return pltpu.make_async_copy(w_o.at[pl.ds(start, d_model), pl.ds(n * QKV_ROWS, QKV_ROWS)], wo_buf.at[n], sem_wo.at[n])

    def gu_copies(layer, step):
        slot = lax.rem(step, FF_SLOTS)
        start = pl.multiple_of(layer * d_model, d_model)
        col = pl.multiple_of(step * FF_TILE, FF_TILE)
        return (
            pltpu.make_async_copy(w_gate.at[pl.ds(start, d_model), pl.ds(col, FF_TILE)], gate_ring.at[slot], sem_ff.at[0, slot]),
            pltpu.make_async_copy(w_up.at[pl.ds(start, d_model), pl.ds(col, FF_TILE)], up_ring.at[slot], sem_ff.at[1, slot]),
        )

    def down_copy(layer, step):
        slot = lax.rem(step, FF_SLOTS)
        start = pl.multiple_of(layer * ff_dim + step * FF_TILE, FF_TILE)
        return pltpu.make_async_copy(w_down.at[pl.ds(start, FF_TILE), :], down_ring.at[slot], sem_ff.at[2, slot])

    def dec_copy(layer, tensor):
        start = pl.multiple_of(layer * d_model + me * LANES, LANES)
        return pltpu.make_async_copy(w_qkv[tensor].at[pl.ds(start, LANES), :], dec_w.at[tensor], sem_dec.at[tensor])

    def block_of(chunk, device):
        return device if chunk == 0 else blocks - 1 - device

    def home(layer, tensor):
        return got_q if tensor == 0 else got.at[layer, tensor - 1]

    def qkv_piece(layer, tensor, chunk, device):
        return remote(
            sent.at[tensor, chunk, device], home(layer, tensor).at[block_of(chunk, me)],
            send_qkv.at[chunk, tensor], recv_qkv.at[layer, chunk, tensor], device,
        )

    def send_to(piece, device):
        @pl.when(device != me)
        def _():
            piece.start()

    def send_queries(layer):
        def body(i, carry):
            qkv_piece(layer, 0, 1, lax.rem(me + 1 + i, group)).start()
            return carry

        lax.fori_loop(0, others, body, 0)

    def send_rest(layer):
        def body(i, carry):
            device = lax.rem(me + 1 + i, group)
            source, place = sent.at[pl.ds(1, 2), 1, device], got.at[layer, pl.ds(0, 2), block_of(1, me)]
            remote(source, place, send_qkv.at[1, 1], recv_qkv.at[layer, 1, 1], device).start()
            return carry

        lax.fori_loop(0, others, body, 0)

    def gain_of(ref, layer):
        gains = ref[...].astype(F32)
        chosen = gains[0:1]
        for n in range(1, num_layers):
            chosen = jnp.where(layer == n, gains[n:n + 1], chosen)
        return chosen

    def normalize(read, row0, count, gain):
        part = 64 if count % 64 == 0 else 48

        def body(i, carry):
            rows = pl.ds(pl.multiple_of(i * part, 16), part)
            wide = read(rows)
            inv = lax.rsqrt(jnp.mean(wide * wide, axis=-1, keepdims=True) + NORM_EPS)
            rows_h[pl.ds(pl.multiple_of(row0 + i * part, 16), part), :] = (wide * inv * gain).astype(BF16)
            return carry

        lax.fori_loop(0, count // part, body, 0)

    def normalize_x(row0, count, gain):
        def read(rows):
            return rows_x[pl.ds(pl.multiple_of(row0 + rows.start, 16), rows.size), :].astype(F32)

        normalize(read, row0, count, gain)

    def rotate(flat, which):
        cosines, sines = tables[2 * which], tables[2 * which + 1]
        heads = flat.reshape(flat.shape[0] // head_dim, head_dim, flat.shape[1])
        first, second = heads[:, :half], heads[:, half:]
        turned = jnp.concatenate([first * cosines - second * sines, second * cosines + first * sines], axis=1)
        return turned.reshape(flat.shape)

    def project(layer, chunk, after_first=None):
        order = order_a if chunk == 0 else order_a[::-1]
        for place, tensor in enumerate(order):
            def body(i, carry, place=place, tensor=tensor):
                spots = (2 * i, 2 * i + 1)
                if chunk == 0 or place > 0:
                    for r in spots:
                        qkv_copy(layer, tensor, r).wait()
                for r in spots:
                    flat = lax.dot_general(
                        qkv_ring[r], rows_h[chunk * blk:(chunk + 1) * blk, :], (((1,), (1,)), ((), ())), preferred_element_type=F32
                    )
                    if tensor != 2:
                        flat = rotate(flat, chunk)
                    sent[tensor, chunk, pl.ds(tile_of(r) * per_tile, per_tile)] = flat.astype(BF16).reshape(per_tile, LANES, blk)
                for r in spots:
                    if place < 2:
                        qkv_copy(layer, order[place + 1], r).start()
                    elif chunk == 1:
                        @pl.when(layer < last)
                        def _(r=r):
                            qkv_copy(layer + 1, order_a[0], r).start()
                    if chunk == 0:
                        for k in range(per_tile):
                            device = tile_of(r) * per_tile + k
                            send_to(qkv_piece(layer, tensor, chunk, device), device)
                return carry

            lax.fori_loop(0, tiles // 2, body, 0)
            home(layer, tensor)[block_of(chunk, me)] = sent[tensor, chunk, me]
            if chunk == 1 and tensor == 0:
                send_queries(layer)
            if place == 0 and after_first is not None:
                after_first()

    def project_decode(layer):
        dec_h[0:PAD] = rows_h[2 * blk:2 * blk + PAD]
        dec_h[head_dim:head_dim + PAD] = rows_h[2 * blk:2 * blk + PAD]
        for tensor in range(3):
            dec_copy(layer, tensor).wait()
            flat = lax.dot_general(dec_w[tensor], dec_h[...], (((1,), (1,)), ((), ())), preferred_element_type=F32)
            if tensor != 2:
                flat = rotate(flat, 2)
            if tensor == 0:
                row = lax.broadcasted_iota(jnp.int32, flat.shape, 0) // head_dim
                col = lax.broadcasted_iota(jnp.int32, flat.shape, 1) // head_dim
                dec_q[...] = jnp.where(row == col, flat, 0.0).astype(BF16)
            elif tensor == 1:
                dec_k[...] = flat.T.astype(BF16)
            else:
                dec_v[...] = flat.astype(BF16)

        @pl.when(layer < last)
        def _():
            for tensor in range(3):
                dec_copy(layer + 1, tensor).start()

    def turn_keys(layer, chunk):
        def body(i, carry):
            for u in range(4):
                j = chunk * group + 4 * i + u
                key_rows[pl.ds(pl.multiple_of(j * blk, blk), blk), :] = got[layer, 0, j].astype(F32).T.astype(BF16)
            return carry

        lax.fori_loop(0, group // 4, body, 0)

    def save_cache(layer, chunk):
        def body(i, carry):
            j = chunk * group + i
            place = pl.ds(pl.multiple_of(j * blk, blk), blk)
            pltpu.make_async_copy(got.at[layer, 0, j], k_cache.at[layer, :, place], sem_cache.at[layer, 0]).start()
            pltpu.make_async_copy(got.at[layer, 1, j], v_cache.at[layer, :, place], sem_cache.at[layer, 1]).start()
            return carry

        lax.fori_loop(0, group, body, 0)

    def scores(layer, pair, tile, slot):
        keys = key_rows[pl.ds(pl.multiple_of(tile * KEY_TILE, KEY_TILE), KEY_TILE), :]
        for u in range(2):
            query = jnp.concatenate([got_q[pair_blocks * pair + 2 * u], got_q[pair_blocks * pair + 2 * u + 1]], axis=1)
            blank = jnp.zeros((head_dim, query.shape[1]), BF16)
            for h in range(heads_dev):
                parts = [blank] * heads_dev
                parts[h] = query[h * head_dim:(h + 1) * head_dim]
                value = jnp.dot(keys, jnp.concatenate(parts, axis=0), preferred_element_type=F32)
                score[slot, 2 * u + h] = value
                best[slot, 2 * u + h] = jnp.max(value, axis=0, keepdims=True)

    def absorb(layer, tile, slot, place, diagonal=False, first=False):
        held = [got[layer, 1, tile * pair_blocks + i] for i in range(pair_blocks)]
        for u in range(2):
            count = pair_blocks // 2 if diagonal and u == 0 else pair_blocks
            ones = jnp.ones((acc_rows - head_dim, count * blk), BF16)
            for h in range(heads_dev):
                c = 2 * u + h
                new = best[slot, c] if first else jnp.maximum(run_max[place, c], best[slot, c])
                probs = jnp.exp2((score[slot, c, :count * blk] - new) * exp_scale).astype(BF16)
                value = jnp.concatenate([jnp.concatenate([b[h * head_dim:(h + 1) * head_dim] for b in held[:count]], axis=1), ones], axis=0)
                added = jnp.dot(value, probs, preferred_element_type=F32)
                if first:
                    run_acc[place, c] = added
                else:
                    run_acc[place, c] = run_acc[place, c] * jnp.exp2((run_max[place, c] - new) * exp_scale) + added
                run_max[place, c] = new

    def mask_diagonal(slot):
        width = score.shape[3]
        key = lax.broadcasted_iota(jnp.int32, (width, width), 0)
        query = lax.broadcasted_iota(jnp.int32, (width, width), 1)
        for u in range(2):
            rows = slice(u * width, (u + 1) * width)
            for h in range(heads_dev):
                c = 2 * u + h
                value = jnp.where(key <= query, score[slot, c, rows], -jnp.inf)
                score[slot, c, rows] = value
                top = jnp.max(value, axis=0, keepdims=True)
                if u == 1:
                    top = jnp.maximum(top, jnp.max(score[slot, c, :width], axis=0, keepdims=True))
                best[slot, c] = top

    def turn_out(place):
        for u in range(2):
            full = jnp.concatenate(
                [run_acc[place, 2 * u + h, :head_dim] / run_acc[place, 2 * u + h, head_dim:head_dim + 1] for h in range(heads_dev)], axis=0
            )
            turned = full.T.astype(BF16)
            for i in range(2):
                mixed_sent[pair_blocks * place + 2 * u + i] = turned[i * blk:(i + 1) * blk]

    def hand_out(layer, chunk, place):
        mine = pl.ds(pl.multiple_of(me * LANES, LANES), LANES)
        for i in range(pair_blocks):
            j = pair_blocks * place + i
            device = j if chunk == 0 else group - 1 - j
            where = mixed.at[chunk * blk:(chunk + 1) * blk, mine]
            send_to(remote(mixed_sent.at[j], where, send_o.at[chunk], recv_o.at[layer, chunk], device), device)

            @pl.when(device == me)
            def _(j=j):
                mixed[chunk * blk:(chunk + 1) * blk, mine] = mixed_sent[j]

    def attend_triangle(layer, chunk):
        base = chunk * pairs
        turn = me // (group // pairs)
        first_slot = [0]
        for pair in range(pairs - 1):
            first_slot.append((first_slot[-1] + pair + 1) % 2)

        def one_pair(pair):
            slot = first_slot[pair]
            for tile in range(pair + 1):
                after = (pair, tile + 1) if tile < pair else ((pair + 1) % pairs, 0)
                scores(layer, base + after[0], base + after[1], 1 - slot)
                if tile == pair:
                    mask_diagonal(slot)
                absorb(layer, base + tile, slot, pair, diagonal=tile == pair, first=tile == 0 and chunk == 0)
                slot = 1 - slot
            turn_out(pair)
            hand_out(layer, chunk, pair)

        for pair in range(pairs):
            @pl.when(turn == pair)
            def _(pair=pair):
                scores(layer, base + pair, base, first_slot[pair])

        def body(i, carry):
            for pair in range(pairs):
                @pl.when(lax.rem(turn + i, pairs) == pair)
                def _(pair=pair):
                    one_pair(pair)
            return carry

        lax.fori_loop(0, pairs, body, 0)

    def attend_square(layer):
        scores(layer, pairs, 0, 0)

        def body(pair, carry):
            for tile in range(pairs):
                if tile + 1 < pairs:
                    scores(layer, pairs + pair, tile + 1, (tile + 1) % 2)
                else:
                    scores(layer, pairs + jnp.minimum(pair + 1, pairs - 1), 0, 0)
                absorb(layer, tile, tile % 2, pair, first=tile == 0)
            return carry

        lax.fori_loop(0, pairs, body, 0)

    def attend_decode(layer):
        ones = jnp.ones((PAD, KEY_TILE), BF16)
        queries = dec_q[...]
        wide = slice(0, LANES)
        spots = [(i // score.shape[1], i % score.shape[1]) for i in range(blocks // pair_blocks)]
        value = jnp.dot(dec_k[...], queries, preferred_element_type=F32)
        key = lax.broadcasted_iota(jnp.int32, value.shape, 0)
        query = lax.rem(lax.broadcasted_iota(jnp.int32, value.shape, 1), head_dim)
        value = jnp.where((key <= query) & (key < steps), value, -jnp.inf)
        top = jnp.max(value, axis=0, keepdims=True)
        for tile, (i, j) in enumerate(spots):
            old = jnp.dot(key_rows[tile * KEY_TILE:(tile + 1) * KEY_TILE, :], queries, preferred_element_type=F32)
            score[i, j, :, wide] = old
            top = jnp.maximum(top, jnp.max(old, axis=0, keepdims=True))
        held = jnp.concatenate([dec_v[...], ones[:, :LANES]], axis=0)
        total = jnp.dot(held, jnp.exp2((value - top) * exp_scale).astype(BF16), preferred_element_type=F32)
        for tile, (i, j) in enumerate(spots):
            held = jnp.concatenate([got[layer, 1, tile * pair_blocks + k] for k in range(pair_blocks)], axis=1)
            probs = jnp.exp2((score[i, j, :, wide] - top) * exp_scale).astype(BF16)
            total = total + jnp.dot(jnp.concatenate([held, ones], axis=0), probs, preferred_element_type=F32)
        turned = (total[:LANES] / total[LANES:LANES + 1]).T
        lane = lax.broadcasted_iota(jnp.int32, (PAD, LANES), 1)
        result = turned[0:PAD]
        for h in range(1, heads_dev):
            result = jnp.where(lane >= h * head_dim, turned[h * head_dim:h * head_dim + PAD], result)
        dec_sent[...] = result.astype(BF16)
        mine = pl.ds(pl.multiple_of(me * LANES, LANES), LANES)
        mixed[2 * blk:2 * blk + PAD, mine] = dec_sent[...]

        def send(i, carry):
            device = lax.rem(me + 1 + i, group)
            remote(dec_sent, mixed.at[2 * blk:2 * blk + PAD, mine], send_d, recv_d.at[layer], device).start()
            return carry

        lax.fori_loop(0, others, send, 0)

    def dense(layer, chunk, between):
        row0, count = (0, blk) if chunk == 0 else (blk, b_rows)
        rows = slice(row0, row0 + count)
        for n in range(tiles):
            if chunk == 0:
                wo_copy(layer, n).wait()
            cols = slice(n * QKV_ROWS, (n + 1) * QKV_ROWS)
            added = rows_x[rows, cols].astype(F32) + jnp.dot(mixed[rows, :], wo_buf[n], preferred_element_type=F32)
            acc[:count, cols] = added.astype(BF16).astype(F32)
        normalize(lambda r: acc[r, :], row0, count, gain_of(gain_mlp, layer))

        def step_at(k):
            return k if chunk == 0 else ff_steps - 1 - k

        def widen(k):
            step = step_at(k)
            slot = lax.rem(step, FF_SLOTS)

            def ready():
                for copy in gu_copies(layer, step):
                    copy.wait()

            if chunk == 0:
                ready()
            else:
                pl.when(k >= FF_SLOTS)(ready)
            normed = rows_h[rows, :]
            gate = jnp.dot(normed, gate_ring[slot], preferred_element_type=F32)
            upward = jnp.dot(normed, up_ring[slot], preferred_element_type=F32)
            gated[:count] = (jax.nn.silu(gate) * upward).astype(BF16)

        def narrow(k):
            step = step_at(k)
            slot = lax.rem(step, FF_SLOTS)

            def ready():
                down_copy(layer, step).wait()

            if chunk == 0:
                ready()
            else:
                pl.when(k >= FF_SLOTS)(ready)
            acc[:count] += jnp.dot(gated[:count], down_ring[slot], preferred_element_type=F32)

        def refill(k, start):
            if chunk == 0:
                @pl.when(k + FF_SLOTS < ff_steps)
                def _():
                    start(layer, k + FF_SLOTS)
            else:
                step = step_at(k)

                @pl.when(step >= FF_SLOTS)
                def _():
                    start(layer, step - FF_SLOTS)

        def start_gu(which, step):
            for copy in gu_copies(which, step):
                copy.start()

        def start_down(which, step):
            down_copy(which, step).start()

        widen(0)
        refill(0, start_gu)

        def body(k, carry):
            narrow(k - 1)
            widen(k)
            refill(k - 1, start_down)
            refill(k, start_gu)
            return carry

        if between is None:
            lax.fori_loop(1, ff_steps, body, 0)
        else:
            split = jnp.where(layer == 0, SPLIT[0], SPLIT[1])
            lax.fori_loop(1, split, body, 0)
            between()
            lax.fori_loop(split, ff_steps, body, 0)
        narrow(ff_steps - 1)
        refill(ff_steps - 1, start_down)
        rows_x[rows, :] = acc[:count].astype(BF16)

    scope = jax.named_scope
    pltpu.make_async_copy(x_in, rows_x.at[0:2 * blk], sem_x).start()
    barrier = pltpu.get_barrier_semaphore()
    for i in range(1, group):
        pl.semaphore_signal(barrier, inc=1, device_id={"cp": lax.rem(me + i, group)}, device_id_type=MESH)
    qkv_copy(0, order_a[0], 0).start()
    dec_h[...] = jnp.zeros_like(dec_h)
    pltpu.make_async_copy(x_in, rows_x.at[0:2 * blk], sem_x).wait()
    for r in range(1, tiles):
        qkv_copy(0, order_a[0], r).start()
    for tensor in range(3):
        dec_copy(0, tensor).start()
    with scope("norm_first"):
        normalize_x(0, 2 * blk, gain_of(gain_attn, 0))
    with scope("barrier"):
        pl.semaphore_wait(barrier, others)

    my_cols = pl.ds(pl.multiple_of(me * LANES, LANES), LANES)

    def part_out(i, carry):
        device = lax.rem(me + 1 + i, group)
        cols = pl.ds(pl.multiple_of(device * LANES, LANES), LANES)
        remote(emb_in.at[:, cols], emb_part.at[me], send_e, recv_e, device).start()
        return carry

    lax.fori_loop(0, others, part_out, 0)
    emb_part[me] = emb_in[:, my_cols]
    def sum_looked_up():
        with scope("embed"):
            wait_recv(emb_part.at[0:others], recv_e)
            emb_sum[...] = jnp.sum(emb_part[...].astype(F32), axis=0).astype(BF16)
            emb_full[:, my_cols] = emb_sum[...]

            def sum_out(i, carry):
                device = lax.rem(me + 1 + i, group)
                remote(emb_sum, emb_full.at[:, my_cols], send_f, recv_f, device).start()
                return carry

            lax.fori_loop(0, others, sum_out, 0)

    with scope("project_first"):
        project(0, 0, sum_looked_up)

    def layer_body(layer, carry):
        with scope("project_b"):
            project(layer, 1)

        for n in range(tiles):
            wo_copy(layer, n).start()
        for step in range(FF_SLOTS):
            for copy in gu_copies(layer, step):
                copy.start()
            down_copy(layer, step).start()

        @pl.when(layer == 0)
        def _():
            wait_recv(emb_part.at[0:others], recv_f)
            rows_x[2 * blk:2 * blk + PAD] = emb_full[...]
            wide = emb_full[...].astype(F32)
            inv = lax.rsqrt(jnp.mean(wide * wide, axis=-1, keepdims=True) + NORM_EPS)
            rows_h[2 * blk:2 * blk + PAD] = (wide * inv * gain_of(gain_attn, 0)).astype(BF16)

        with scope("project_dec"):
            project_decode(layer)
        with scope("wait_a"):
            for tensor in range(3):
                wait_recv(home(layer, tensor).at[0:others], recv_qkv.at[layer, 0, tensor])
        with scope("attend_aa"):
            turn_keys(layer, 0)
            save_cache(layer, 0)
            attend_triangle(layer, 0)
        send_rest(layer)
        with scope("wait_q"):
            wait_recv(got_q.at[0:others], recv_qkv.at[layer, 1, 0])
        with scope("attend_ba"):
            attend_square(layer)
        with scope("wait_oa"):
            for tensor in range(3):
                wait_send(sent.at[tensor, 0, 0:others], send_qkv.at[0, tensor])
            wait_recv(mixed_sent.at[0:others], recv_o.at[layer, 0])

        def finish_attention():
            with scope("wait_kv"):
                wait_recv(got.at[layer, pl.ds(0, 2), pl.ds(0, others)], recv_qkv.at[layer, 1, 1])
            wait_send(mixed_sent.at[0:others], send_o.at[0])
            with scope("attend_bb"):
                turn_keys(layer, 1)
                attend_triangle(layer, 1)
            with scope("attend_dec"):
                attend_decode(layer)
                save_cache(layer, 1)

        with scope("dense_a"):
            dense(layer, 0, finish_attention)
        with scope("drain_a"):
            wait_send(sent.at[0, 1, 0:others], send_qkv.at[1, 0])
            wait_send(sent.at[pl.ds(1, 2), 1, pl.ds(0, others)], send_qkv.at[1, 1])

        @pl.when(layer < last)
        def _():
            with scope("project_a"):
                normalize_x(0, blk, gain_of(gain_attn, layer + 1))
                project(layer + 1, 0)

        @pl.when(layer == last)
        def _():
            pltpu.make_async_copy(rows_x.at[0:blk], x_out.at[0:blk], sem_out.at[0]).start()

        with scope("wait_ob"):
            wait_recv(mixed_sent.at[0:others], recv_o.at[layer, 1])
            wait_recv(emb_part.at[0:others], recv_d.at[layer])
        with scope("dense_b"):
            dense(layer, 1, None)
        with scope("drain_b"):
            wait_send(mixed_sent.at[0:others], send_o.at[1])
            wait_send(emb_part.at[0:others], send_d)

        @pl.when(layer < last)
        def _():
            normalize_x(blk, b_rows, gain_of(gain_attn, layer + 1))

        return carry

    lax.fori_loop(0, num_layers, layer_body, 0)

    pltpu.make_async_copy(rows_x.at[blk:2 * blk], x_out.at[blk:2 * blk], sem_out.at[1]).start()
    dec_out[...] = rows_x[2 * blk:2 * blk + PAD]
    wait_send(emb_part.at[0:others], send_e)
    wait_send(emb_part.at[0:others], send_f)
    for layer in range(num_layers):
        pltpu.make_async_copy(k_cache.at[layer], k_cache.at[layer], sem_cache.at[layer, 0]).wait()
        pltpu.make_async_copy(v_cache.at[layer], v_cache.at[layer], sem_cache.at[layer, 1]).wait()
    for part in range(2):
        where = pl.ds(part * blk, blk)
        pltpu.make_async_copy(rows_x.at[where], x_out.at[where], sem_out.at[part]).wait()


def place_kernel(x_ref, k_ref, v_ref, dec_ref, x_to, k_to, v_to, dec_to, x_held, k_held, v_held, dec_held, sems):
    moves = ((k_ref, k_held, k_to), (v_ref, v_held, v_to), (x_ref, x_held, x_to))
    for n, (source, held, _) in enumerate(moves):
        pltpu.make_async_copy(source, held, sems.at[0, n]).start()
    pltpu.make_async_copy(dec_ref, dec_held, sems.at[0, 3]).start()
    for n, (source, held, result) in enumerate(moves):
        pltpu.make_async_copy(source, held, sems.at[0, n]).wait()
        pltpu.make_async_copy(held, result, sems.at[1, n]).start()
    pltpu.make_async_copy(dec_ref, dec_held, sems.at[0, 3]).wait()
    dec_to[...] = dec_held[0:dec_to.shape[0]]
    for n, (_, held, result) in enumerate(moves):
        pltpu.make_async_copy(held, result, sems.at[1, n]).wait()


def place(steps, *arrays):
    spec = pl.BlockSpec(memory_space=pl.ANY)
    shapes = [jax.ShapeDtypeStruct(a.shape, a.dtype) for a in arrays]
    shapes[-1] = jax.ShapeDtypeStruct((steps,) + arrays[-1].shape[1:], arrays[-1].dtype)
    return pl.pallas_call(
        place_kernel,
        out_shape=tuple(shapes),
        in_specs=[spec] * len(arrays),
        out_specs=(spec, spec, spec, pl.BlockSpec(memory_space=pltpu.VMEM)),
        scratch_shapes=[pltpu.VMEM(a.shape, a.dtype) for a in arrays] + [pltpu.SemaphoreType.DMA((2, len(arrays)))],
        compiler_params=pltpu.CompilerParams(vmem_limit_bytes=67_000_000),
        name="place",
    )(*arrays)


def solution(mesh):
    group = mesh.shape["cp"]

    def local_program(x_rows, token_ids, table_rows, norm_attn, w_q, w_k, w_v, w_o, norm_mlp, w_gate, w_up, w_down):
        device = lax.axis_index("cp")
        num_layers, d_model, num_heads, head_dim = w_q.shape
        kv_heads = w_k.shape[2]
        ff_dim = w_gate.shape[2]
        seq_dev = x_rows.shape[0]
        blk = seq_dev // 2
        seq_len = group * seq_dev
        steps = token_ids.shape[0]
        heads_dev = num_heads // group
        assert heads_dev * head_dim == LANES and kv_heads == num_heads and blk == LANES

        emb = pick_rows(token_ids, (device * table_rows.shape[0]).reshape(1), table_rows)

        offsets = jnp.arange(LANES, dtype=jnp.int32)
        positions = jnp.stack([device * blk + offsets, (2 * group - 1 - device) * blk + offsets, seq_len + offsets % head_dim])
        inv_freq = 1.0 / (ROPE_BASE ** (jnp.arange(0, head_dim, 2, dtype=F32) / head_dim))
        angles = positions.astype(F32)[:, None, :] * inv_freq[None, :, None]
        tables = jnp.stack([jnp.cos(angles), jnp.sin(angles)], axis=1).reshape(6, head_dim // 2, LANES)

        def head_rows(w):
            return w.transpose(0, 2, 3, 1).reshape(num_layers * num_heads * head_dim, d_model)

        any_spec = pl.BlockSpec(memory_space=pl.ANY)
        vmem = pl.BlockSpec(memory_space=pltpu.VMEM)
        dma = pltpu.SemaphoreType.DMA
        acc_rows = head_dim + 8
        quarter = KEY_TILE // 2
        tiles = d_model // QKV_ROWS
        pairs = group * blk // KEY_TILE
        scratch = [
            pltpu.VMEM((2 * blk + PAD, d_model), BF16),
            pltpu.VMEM((2 * blk + PAD, d_model), BF16),
            pltpu.VMEM((2 * blk + PAD, d_model), BF16),
            pltpu.VMEM((3, 2, group, LANES, blk), BF16),
            pltpu.VMEM((2 * group, LANES, blk), BF16),
            pltpu.VMEM((num_layers, 2, 2 * group, LANES, blk), BF16),
            pltpu.VMEM((seq_len, LANES), BF16),
            pltpu.VMEM((group, blk, LANES), BF16),
            pltpu.VMEM((2, 2 * heads_dev, KEY_TILE, quarter), F32),
            pltpu.VMEM((2, 2 * heads_dev, 1, quarter), F32),
            pltpu.VMEM((pairs, 2 * heads_dev, 1, quarter), F32),
            pltpu.VMEM((pairs, 2 * heads_dev, acc_rows, quarter), F32),
            pltpu.VMEM((tiles, QKV_ROWS, d_model), BF16),
            pltpu.VMEM((tiles, d_model, QKV_ROWS), BF16),
            pltpu.VMEM((FF_SLOTS, d_model, FF_TILE), BF16),
            pltpu.VMEM((FF_SLOTS, d_model, FF_TILE), BF16),
            pltpu.VMEM((FF_SLOTS, FF_TILE, d_model), BF16),
            pltpu.VMEM((3, LANES, d_model), BF16),
            pltpu.VMEM((LANES, d_model), BF16),
            pltpu.VMEM((LANES, LANES), BF16),
            pltpu.VMEM((LANES, LANES), BF16),
            pltpu.VMEM((LANES, LANES), BF16),
            pltpu.VMEM((blk + PAD, d_model), F32),
            pltpu.VMEM((blk + PAD, FF_TILE), BF16),
            pltpu.VMEM((group, PAD, LANES), BF16),
            pltpu.VMEM((PAD, d_model), BF16),
            pltpu.VMEM((PAD, LANES), BF16),
            pltpu.VMEM((PAD, LANES), BF16),
            dma, dma((tiles,)), dma((tiles,)), dma((3, FF_SLOTS)), dma((3,)),
            dma((2, 3)), dma((num_layers, 2, 3)), dma((2,)), dma((num_layers, 2)), dma, dma((num_layers,)),
            dma, dma, dma, dma, dma((num_layers, 2)), dma((2,)),
        ]
        x_new, k_flat, v_flat, dec = pl.pallas_call(
            functools.partial(main_kernel, group, head_dim, num_layers, steps),
            out_shape=(
                jax.ShapeDtypeStruct((seq_dev, d_model), BF16),
                jax.ShapeDtypeStruct((num_layers, LANES, seq_len), BF16),
                jax.ShapeDtypeStruct((num_layers, LANES, seq_len), BF16),
                jax.ShapeDtypeStruct((PAD, d_model), BF16),
            ),
            in_specs=[any_spec, vmem, vmem, vmem, vmem] + [any_spec] * 7,
            out_specs=(any_spec, any_spec, any_spec, vmem),
            scratch_shapes=scratch,
            compiler_params=pltpu.CompilerParams(collective_id=0, has_side_effects=True, vmem_limit_bytes=67_000_000),
            name="prefill_decode",
        )(
            x_rows, emb, norm_attn, norm_mlp, tables,
            head_rows(w_q), head_rows(w_k), head_rows(w_v), w_o.reshape(num_layers * d_model, d_model),
            w_gate.reshape(num_layers * d_model, ff_dim), w_up.reshape(num_layers * d_model, ff_dim), w_down.reshape(num_layers * ff_dim, d_model),
        )

        def cache(flat):
            return flat.reshape(num_layers, heads_dev, head_dim, seq_len).transpose(0, 3, 1, 2)

        x_new, k_flat, v_flat, dec = place(steps, x_new, k_flat, v_flat, dec)
        return x_new, cache(k_flat), cache(v_flat), dec

    replicated = P()
    in_specs = (P(("req", "cp"), None), P("req"), P("cp", None)) + (replicated,) * 9
    out_specs = (P(("req", "cp"), None), P(None, "req", "cp", None), P(None, "req", "cp", None), P("req", None))
    return jax.shard_map(local_program, mesh=mesh, in_specs=in_specs, out_specs=out_specs, check_vma=False)
```

```python
import functools

import jax
import jax.numpy as jnp
from jax import lax
from jax.experimental import pallas as pl
from jax.experimental.pallas import tpu as pltpu
from jax.sharding import PartitionSpec as P

ROPE_BASE = 10000.0
NORM_EPS = 1e-5
LOG2_E = 1.4426950408889634
BF16 = jnp.bfloat16
F32 = jnp.float32
MESH = pl.DeviceIdType.MESH
LANES = 128
PAD = 16
QKV_ROWS = 512
FF_TILE = 512
FF_SLOTS = 4
KEY_TILE = 512
SPLIT = (14, 12)


def pick_kernel(vocab_dev, ids_ref, table_ref, out_ref, rows, sems):
    steps = ids_ref.shape[0]
    base = lax.axis_index("cp") * vocab_dev

    def copy(t):
        local = jnp.clip(ids_ref[t] - base, 0, vocab_dev - 1)
        start = pl.multiple_of((local // 8) * 8, 8)
        return pltpu.make_async_copy(table_ref.at[pl.ds(start, 8), :], rows.at[t], sems.at[t])

    for t in range(steps):
        copy(t).start()
    out_ref[...] = jnp.zeros_like(out_ref)
    picked = []
    for t in range(steps):
        copy(t).wait()
        local = ids_ref[t] - base
        inside = (local >= 0) & (local < vocab_dev)
        which = jnp.where(inside, lax.rem(jnp.clip(local, 0, vocab_dev - 1), 8), -1)
        index = lax.broadcasted_iota(jnp.int32, rows.shape[1:], 0)
        picked.append(jnp.sum(jnp.where(index == which, rows[t].astype(F32), 0.0), axis=0, keepdims=True))
    picked.append(jnp.zeros((PAD - steps, rows.shape[2]), F32))
    out_ref[...] = jnp.concatenate(picked, axis=0).astype(BF16)


def pick_rows(token_ids, table_rows):
    vocab_dev, d_model = table_rows.shape
    steps = token_ids.shape[0]
    return pl.pallas_call(
        functools.partial(pick_kernel, vocab_dev),
        out_shape=jax.ShapeDtypeStruct((PAD, d_model), BF16),
        in_specs=[
            pl.BlockSpec(memory_space=pltpu.SMEM),
            pl.BlockSpec(memory_space=pl.ANY),
        ],
        out_specs=pl.BlockSpec(memory_space=pltpu.VMEM),
        scratch_shapes=[pltpu.VMEM((steps, 8, d_model), BF16), pltpu.SemaphoreType.DMA((steps,))],
        name="pick_rows",
    )(token_ids, table_rows)


def main_kernel(
    group, head_dim, num_layers, steps,
    x_in, emb_in, gain_attn, gain_mlp, tables, w_q, w_k, w_v, w_o, w_gate, w_up, w_down,
    x_out, k_cache, v_cache, dec_out,
    rows_x, rows_h, mixed, sent, got_q, got, key_rows, mixed_sent, score, best, run_max, run_acc,
    qkv_ring, wo_buf, gate_ring, up_ring, down_ring, dec_w, dec_q, dec_k, dec_v, acc, gated, emb_part, emb_sum, dec_sent,
    sem_x, sem_qkv, sem_wo, sem_ff, sem_dec, send_qkv, recv_qkv, send_o, recv_o, send_d, recv_d, send_e, recv_e, send_f, recv_f, sem_cache, sem_out,
):
    me = lax.axis_index("cp")
    blk = LANES
    blocks = 2 * group
    d_model = rows_x.shape[1]
    ff_dim = w_gate.shape[1]
    ff_steps = ff_dim // FF_TILE
    heads_dev = LANES // head_dim
    per_tile = QKV_ROWS // LANES
    tiles = d_model // QKV_ROWS
    half = head_dim // 2
    pair_blocks = KEY_TILE // blk
    pairs = group // pair_blocks
    exp_scale = float(head_dim ** -0.5 * LOG2_E)
    acc_rows = run_acc.shape[2]
    last = num_layers - 1
    b_rows = blk + PAD
    others = group - 1
    neighbour = lax.rem(me + 1, group)
    w_qkv = (w_q, w_k, w_v)
    order_a = (1, 2, 0)

    def remote(src, dst, ssem, rsem, device):
        return pltpu.make_async_remote_copy(src_ref=src, dst_ref=dst, send_sem=ssem, recv_sem=rsem, device_id={"cp": device}, device_id_type=MESH)

    def wait_recv(ref, sem):
        remote(ref, ref, send_e, sem, neighbour).wait_recv()

    def wait_send(ref, sem):
        remote(ref, ref, sem, recv_e, neighbour).wait_send()

    def tile_of(r):
        return lax.rem(r + me // per_tile + 1, tiles)

    def qkv_copy(layer, tensor, r):
        start = pl.multiple_of(layer * d_model + tile_of(r) * QKV_ROWS, QKV_ROWS)
        return pltpu.make_async_copy(w_qkv[tensor].at[pl.ds(start, QKV_ROWS), :], qkv_ring.at[r], sem_qkv.at[r])

    def wo_copy(layer, n):
        start = pl.multiple_of(layer * d_model, d_model)
        return pltpu.make_async_copy(w_o.at[pl.ds(start, d_model), pl.ds(n * QKV_ROWS, QKV_ROWS)], wo_buf.at[n], sem_wo.at[n])

    def gu_copies(layer, step):
        slot = lax.rem(step, FF_SLOTS)
        start = pl.multiple_of(layer * d_model, d_model)
        col = pl.multiple_of(step * FF_TILE, FF_TILE)
        return (
            pltpu.make_async_copy(w_gate.at[pl.ds(start, d_model), pl.ds(col, FF_TILE)], gate_ring.at[slot], sem_ff.at[0, slot]),
            pltpu.make_async_copy(w_up.at[pl.ds(start, d_model), pl.ds(col, FF_TILE)], up_ring.at[slot], sem_ff.at[1, slot]),
        )

    def down_copy(layer, step):
        slot = lax.rem(step, FF_SLOTS)
        start = pl.multiple_of(layer * ff_dim + step * FF_TILE, FF_TILE)
        return pltpu.make_async_copy(w_down.at[pl.ds(start, FF_TILE), :], down_ring.at[slot], sem_ff.at[2, slot])

    def dec_copy(layer, tensor):
        start = pl.multiple_of(layer * d_model + me * LANES, LANES)
        return pltpu.make_async_copy(w_qkv[tensor].at[pl.ds(start, LANES), :], dec_w.at[tensor], sem_dec.at[tensor])

    def block_of(chunk, device):
        return device if chunk == 0 else blocks - 1 - device

    def home(layer, tensor):
        return got_q if tensor == 0 else got.at[layer, tensor - 1]

    def qkv_piece(layer, tensor, chunk, device):
        return remote(
            sent.at[tensor, chunk, device], home(layer, tensor).at[block_of(chunk, me)],
            send_qkv.at[chunk, tensor], recv_qkv.at[layer, chunk, tensor], device,
        )

    def send_to(piece, device):
        @pl.when(device != me)
        def _():
            piece.start()

    def send_queries(layer):
        def body(i, carry):
            qkv_piece(layer, 0, 1, lax.rem(me + 1 + i, group)).start()
            return carry

        lax.fori_loop(0, others, body, 0)

    def send_rest(layer):
        def body(i, carry):
            device = lax.rem(me + 1 + i, group)
            source, place = sent.at[pl.ds(1, 2), 1, device], got.at[layer, pl.ds(0, 2), block_of(1, me)]
            remote(source, place, send_qkv.at[1, 1], recv_qkv.at[layer, 1, 1], device).start()
            return carry

        lax.fori_loop(0, others, body, 0)

    def gain_of(ref, layer):
        gains = ref[...].astype(F32)
        chosen = gains[0:1]
        for n in range(1, num_layers):
            chosen = jnp.where(layer == n, gains[n:n + 1], chosen)
        return chosen

    def normalize(read, row0, count, gain):
        part = 64 if count % 64 == 0 else 48

        def body(i, carry):
            rows = pl.ds(pl.multiple_of(i * part, 16), part)
            wide = read(rows)
            inv = lax.rsqrt(jnp.mean(wide * wide, axis=-1, keepdims=True) + NORM_EPS)
            rows_h[pl.ds(pl.multiple_of(row0 + i * part, 16), part), :] = (wide * inv * gain).astype(BF16)
            return carry

        lax.fori_loop(0, count // part, body, 0)

    def normalize_x(row0, count, gain):
        def read(rows):
            return rows_x[pl.ds(pl.multiple_of(row0 + rows.start, 16), rows.size), :].astype(F32)

        normalize(read, row0, count, gain)

    def rotate(flat, which):
        cosines, sines = tables[2 * which], tables[2 * which + 1]
        heads = flat.reshape(flat.shape[0] // head_dim, head_dim, flat.shape[1])
        first, second = heads[:, :half], heads[:, half:]
        turned = jnp.concatenate([first * cosines - second * sines, second * cosines + first * sines], axis=1)
        return turned.reshape(flat.shape)

    def project(layer, chunk, between=()):
        order = order_a if chunk == 0 else order_a[::-1]
        for place, tensor in enumerate(order):
            def body(i, carry, place=place, tensor=tensor):
                spots = (2 * i, 2 * i + 1)
                if chunk == 0 or place > 0:
                    for r in spots:
                        qkv_copy(layer, tensor, r).wait()
                for r in spots:
                    flat = lax.dot_general(
                        qkv_ring[r], rows_h[chunk * blk:(chunk + 1) * blk, :], (((1,), (1,)), ((), ())), preferred_element_type=F32
                    )
                    if tensor != 2:
                        flat = rotate(flat, chunk)
                    sent[tensor, chunk, pl.ds(tile_of(r) * per_tile, per_tile)] = flat.astype(BF16).reshape(per_tile, LANES, blk)
                for r in spots:
                    if place < 2:
                        qkv_copy(layer, order[place + 1], r).start()
                    elif chunk == 1:
                        @pl.when(layer < last)
                        def _(r=r):
                            qkv_copy(layer + 1, order_a[0], r).start()
                    if chunk == 0:
                        for k in range(per_tile):
                            device = tile_of(r) * per_tile + k
                            send_to(qkv_piece(layer, tensor, chunk, device), device)
                return carry

            lax.fori_loop(0, tiles // 2, body, 0)
            home(layer, tensor)[block_of(chunk, me)] = sent[tensor, chunk, me]
            if chunk == 1 and tensor == 0:
                send_queries(layer)
            if place < len(between):
                between[place]()

    def project_decode(layer):
        few = rows_h[2 * blk:2 * blk + PAD]
        blank = jnp.zeros((head_dim - PAD, d_model), BF16)
        normed = jnp.concatenate([few, blank] * heads_dev, axis=0)
        for tensor in range(3):
            dec_copy(layer, tensor).wait()
            flat = lax.dot_general(dec_w[tensor], normed, (((1,), (1,)), ((), ())), preferred_element_type=F32)
            if tensor != 2:
                flat = rotate(flat, 2)
            if tensor == 0:
                row = lax.broadcasted_iota(jnp.int32, flat.shape, 0) // head_dim
                col = lax.broadcasted_iota(jnp.int32, flat.shape, 1) // head_dim
                dec_q[...] = jnp.where(row == col, flat, 0.0).astype(BF16)
            elif tensor == 1:
                dec_k[...] = flat.T.astype(BF16)
            else:
                dec_v[...] = flat.astype(BF16)

        @pl.when(layer < last)
        def _():
            for tensor in range(3):
                dec_copy(layer + 1, tensor).start()

    def turn_keys(layer, chunk):
        def body(i, carry):
            for u in range(4):
                j = chunk * group + 4 * i + u
                key_rows[pl.ds(pl.multiple_of(j * blk, blk), blk), :] = got[layer, 0, j].astype(F32).T.astype(BF16)
            return carry

        lax.fori_loop(0, group // 4, body, 0)

    def save_cache(layer, chunk):
        def body(i, carry):
            j = chunk * group + i
            place = pl.ds(pl.multiple_of(j * blk, blk), blk)
            pltpu.make_async_copy(got.at[layer, 0, j], k_cache.at[layer, :, place], sem_cache.at[layer, 0]).start()
            pltpu.make_async_copy(got.at[layer, 1, j], v_cache.at[layer, :, place], sem_cache.at[layer, 1]).start()
            return carry

        lax.fori_loop(0, group, body, 0)

    def scores(layer, pair, tile, slot):
        keys = key_rows[pl.ds(pl.multiple_of(tile * KEY_TILE, KEY_TILE), KEY_TILE), :]
        for u in range(2):
            query = jnp.concatenate([got_q[pair_blocks * pair + 2 * u], got_q[pair_blocks * pair + 2 * u + 1]], axis=1)
            blank = jnp.zeros((head_dim, query.shape[1]), BF16)
            for h in range(heads_dev):
                parts = [blank] * heads_dev
                parts[h] = query[h * head_dim:(h + 1) * head_dim]
                value = jnp.dot(keys, jnp.concatenate(parts, axis=0), preferred_element_type=F32)
                score[slot, 2 * u + h] = value
                best[slot, 2 * u + h] = jnp.max(value, axis=0, keepdims=True)

    def absorb(layer, tile, slot, place, diagonal=False, first=False):
        held = [got[layer, 1, tile * pair_blocks + i] for i in range(pair_blocks)]
        for u in range(2):
            count = pair_blocks // 2 if diagonal and u == 0 else pair_blocks
            ones = jnp.ones((acc_rows - head_dim, count * blk), BF16)
            for h in range(heads_dev):
                c = 2 * u + h
                new = best[slot, c] if first else jnp.maximum(run_max[place, c], best[slot, c])
                probs = jnp.exp2((score[slot, c, :count * blk] - new) * exp_scale).astype(BF16)
                value = jnp.concatenate([jnp.concatenate([b[h * head_dim:(h + 1) * head_dim] for b in held[:count]], axis=1), ones], axis=0)
                added = jnp.dot(value, probs, preferred_element_type=F32)
                if first:
                    run_acc[place, c] = added
                else:
                    run_acc[place, c] = run_acc[place, c] * jnp.exp2((run_max[place, c] - new) * exp_scale) + added
                run_max[place, c] = new

    def mask_diagonal(slot):
        width = score.shape[3]
        key = lax.broadcasted_iota(jnp.int32, (width, width), 0)
        query = lax.broadcasted_iota(jnp.int32, (width, width), 1)
        for u in range(2):
            rows = slice(u * width, (u + 1) * width)
            for h in range(heads_dev):
                c = 2 * u + h
                value = jnp.where(key <= query, score[slot, c, rows], -jnp.inf)
                score[slot, c, rows] = value
                top = jnp.max(value, axis=0, keepdims=True)
                if u == 1:
                    top = jnp.maximum(top, jnp.max(score[slot, c, :width], axis=0, keepdims=True))
                best[slot, c] = top

    def turn_out(place):
        for u in range(2):
            full = jnp.concatenate(
                [run_acc[place, 2 * u + h, :head_dim] / run_acc[place, 2 * u + h, head_dim:head_dim + 1] for h in range(heads_dev)], axis=0
            )
            turned = full.T.astype(BF16)
            for i in range(2):
                mixed_sent[pair_blocks * place + 2 * u + i] = turned[i * blk:(i + 1) * blk]

    def hand_out(layer, chunk, place):
        for i in range(pair_blocks):
            j = pair_blocks * place + i
            device = j if chunk == 0 else group - 1 - j
            where = mixed.at[me, chunk * blk:(chunk + 1) * blk]
            send_to(remote(mixed_sent.at[j], where, send_o.at[chunk], recv_o.at[layer, chunk], device), device)

            @pl.when(device == me)
            def _(j=j):
                mixed[me, chunk * blk:(chunk + 1) * blk] = mixed_sent[j]

    def attend_triangle(layer, chunk, middle=None):
        base = chunk * pairs
        quarter = me // (group // pairs)
        turn = lax.rem(quarter + 1 if chunk == 0 else pairs - quarter, pairs)
        first_slot = [0]
        for pair in range(pairs - 1):
            first_slot.append((first_slot[-1] + pair + 1) % 2)

        def one_pair(pair, i):
            slot = first_slot[pair]
            then = jnp.where(i == pairs - 1, pair, (pair + 1) % pairs)
            for tile in range(pair + 1):
                after = (pair, tile + 1) if tile < pair else (then, 0)
                scores(layer, base + after[0], base + after[1], 1 - slot)
                if tile == pair:
                    mask_diagonal(slot)
                absorb(layer, base + tile, slot, pair, diagonal=tile == pair, first=tile == 0 and chunk == 0)
                slot = 1 - slot
            turn_out(pair)
            hand_out(layer, chunk, pair)

        for pair in range(pairs):
            @pl.when(turn == pair)
            def _(pair=pair):
                scores(layer, base + pair, base, first_slot[pair])

        def body(i, carry):
            for pair in range(pairs):
                @pl.when(lax.rem(turn + i, pairs) == pair)
                def _(pair=pair):
                    one_pair(pair, i)
            if middle is not None:
                pl.when(i == pairs // 2 - 1)(middle)
            return carry

        lax.fori_loop(0, pairs, body, 0)

    def attend_square(layer):
        scores(layer, pairs, 0, 0)

        def body(pair, carry):
            for tile in range(pairs):
                if tile + 1 < pairs:
                    scores(layer, pairs + pair, tile + 1, (tile + 1) % 2)
                else:
                    scores(layer, pairs + jnp.minimum(pair + 1, pairs - 1), 0, 0)
                absorb(layer, tile, tile % 2, pair, first=tile == 0)

            @pl.when(pair == jnp.where(layer == 0, pairs - 1, pairs - 2))
            def _():
                send_rest(layer)

            return carry

        lax.fori_loop(0, pairs, body, 0)

    def attend_decode(layer):
        ones = jnp.ones((PAD, KEY_TILE), BF16)
        queries = dec_q[...]
        value = jnp.dot(dec_k[...], queries, preferred_element_type=F32)
        key = lax.broadcasted_iota(jnp.int32, value.shape, 0)
        query = lax.rem(lax.broadcasted_iota(jnp.int32, value.shape, 1), head_dim)
        value = jnp.where((key <= query) & (key < steps), value, -jnp.inf)
        top = jnp.max(value, axis=0, keepdims=True)

        def old(tile):
            return jnp.dot(key_rows[tile * KEY_TILE:(tile + 1) * KEY_TILE, :], queries, preferred_element_type=F32)

        for tile in range(blocks // pair_blocks):
            top = jnp.maximum(top, jnp.max(old(tile), axis=0, keepdims=True))
        held = jnp.concatenate([dec_v[...], ones[:, :LANES]], axis=0)
        total = jnp.dot(held, jnp.exp2((value - top) * exp_scale).astype(BF16), preferred_element_type=F32)
        for tile in range(blocks // pair_blocks):
            held = jnp.concatenate([got[layer, 1, tile * pair_blocks + k] for k in range(pair_blocks)], axis=1)
            probs = jnp.exp2((old(tile) - top) * exp_scale).astype(BF16)
            total = total + jnp.dot(jnp.concatenate([held, ones], axis=0), probs, preferred_element_type=F32)
        turned = (total[:LANES] / total[LANES:LANES + 1]).T
        lane = lax.broadcasted_iota(jnp.int32, (PAD, LANES), 1)
        result = turned[0:PAD]
        for h in range(1, heads_dev):
            result = jnp.where(lane >= h * head_dim, turned[h * head_dim:h * head_dim + PAD], result)
        dec_sent[...] = result.astype(BF16)
        mixed[me, 2 * blk:2 * blk + PAD] = dec_sent[...]

        def send(i, carry):
            device = lax.rem(me + 1 + i, group)
            remote(dec_sent, mixed.at[me, 2 * blk:2 * blk + PAD], send_d, recv_d.at[layer], device).start()
            return carry

        lax.fori_loop(0, others, send, 0)

    def dense(layer, chunk, between):
        row0, count = (0, blk) if chunk == 0 else (blk, b_rows)
        rows = slice(row0, row0 + count)
        heads = jnp.concatenate([mixed[n, rows] for n in range(group)], axis=1)
        for n in range(tiles):
            if chunk == 0:
                wo_copy(layer, n).wait()
            cols = slice(n * QKV_ROWS, (n + 1) * QKV_ROWS)
            added = rows_x[rows, cols].astype(F32) + jnp.dot(heads, wo_buf[n], preferred_element_type=F32)
            acc[:count, cols] = added.astype(BF16).astype(F32)
        normalize(lambda r: acc[r, :], row0, count, gain_of(gain_mlp, layer))

        def step_at(k):
            return k if chunk == 0 else ff_steps - 1 - k

        def widen(k):
            step = step_at(k)
            slot = lax.rem(step, FF_SLOTS)

            def ready():
                for copy in gu_copies(layer, step):
                    copy.wait()

            if chunk == 0:
                ready()
            else:
                pl.when(k >= FF_SLOTS)(ready)
            normed = rows_h[rows, :]
            gate = jnp.dot(normed, gate_ring[slot], preferred_element_type=F32)
            upward = jnp.dot(normed, up_ring[slot], preferred_element_type=F32)
            gated[:count] = (jax.nn.silu(gate) * upward).astype(BF16)

        def narrow(k):
            step = step_at(k)
            slot = lax.rem(step, FF_SLOTS)

            def ready():
                down_copy(layer, step).wait()

            if chunk == 0:
                ready()
            else:
                pl.when(k >= FF_SLOTS)(ready)
            acc[:count] += jnp.dot(gated[:count], down_ring[slot], preferred_element_type=F32)

        def refill(k, start):
            if chunk == 0:
                @pl.when(k + FF_SLOTS < ff_steps)
                def _():
                    start(layer, k + FF_SLOTS)
            else:
                step = step_at(k)

                @pl.when(step >= FF_SLOTS)
                def _():
                    start(layer, step - FF_SLOTS)

        def start_gu(which, step):
            for copy in gu_copies(which, step):
                copy.start()

        def start_down(which, step):
            down_copy(which, step).start()

        widen(0)
        refill(0, start_gu)

        def body(k, carry):
            narrow(k - 1)
            widen(k)
            refill(k - 1, start_down)
            refill(k, start_gu)
            return carry

        if between is None:
            lax.fori_loop(1, ff_steps, body, 0)
        else:
            split = jnp.where(layer == 0, SPLIT[0], SPLIT[1])
            lax.fori_loop(1, split, body, 0)
            between()
            lax.fori_loop(split, ff_steps, body, 0)
        narrow(ff_steps - 1)
        refill(ff_steps - 1, start_down)
        rows_x[rows, :] = acc[:count].astype(BF16)

    scope = jax.named_scope
    pltpu.make_async_copy(x_in, rows_x.at[0:2 * blk], sem_x).start()
    barrier = pltpu.get_barrier_semaphore()
    for i in range(1, group):
        pl.semaphore_signal(barrier, inc=1, device_id={"cp": lax.rem(me + i, group)}, device_id_type=MESH)
    qkv_copy(0, order_a[0], 0).start()
    pltpu.make_async_copy(x_in, rows_x.at[0:2 * blk], sem_x).wait()
    for r in range(1, tiles):
        qkv_copy(0, order_a[0], r).start()
    for tensor in range(3):
        dec_copy(0, tensor).start()
    with scope("norm_first"):
        normalize_x(0, blk, gain_of(gain_attn, 0))
    with scope("barrier"):
        pl.semaphore_wait(barrier, others)

    my_cols = pl.ds(pl.multiple_of(me * LANES, LANES), LANES)

    def split_looked_up():
        def part_out(i, carry):
            device = lax.rem(me + 1 + i, group)
            cols = pl.ds(pl.multiple_of(device * LANES, LANES), LANES)
            remote(emb_in.at[:, cols], emb_part.at[me], send_e, recv_e, device).start()
            return carry

        lax.fori_loop(0, others, part_out, 0)
        emb_part[me] = emb_in[:, my_cols]

    def sum_looked_up():
        with scope("embed"):
            wait_recv(emb_part.at[0:others], recv_e)
            emb_sum[...] = jnp.sum(emb_part[...].astype(F32), axis=0).astype(BF16)
            rows_x[2 * blk:2 * blk + PAD, my_cols] = emb_sum[...]

            def sum_out(i, carry):
                device = lax.rem(me + 1 + i, group)
                remote(emb_sum, rows_x.at[2 * blk:2 * blk + PAD, my_cols], send_f, recv_f, device).start()
                return carry

            lax.fori_loop(0, others, sum_out, 0)

    with scope("project_first"):
        project(0, 0, (split_looked_up, sum_looked_up))
        normalize_x(blk, blk, gain_of(gain_attn, 0))

    def layer_body(layer, carry):
        with scope("project_b"):
            project(layer, 1)

        for n in range(tiles):
            wo_copy(layer, n).start()
        for step in range(FF_SLOTS):
            for copy in gu_copies(layer, step):
                copy.start()
            down_copy(layer, step).start()

        @pl.when(layer == 0)
        def _():
            wait_recv(emb_part.at[0:others], recv_f)
            wide = rows_x[2 * blk:2 * blk + PAD].astype(F32)
            inv = lax.rsqrt(jnp.mean(wide * wide, axis=-1, keepdims=True) + NORM_EPS)
            rows_h[2 * blk:2 * blk + PAD] = (wide * inv * gain_of(gain_attn, 0)).astype(BF16)
            with scope("project_dec"):
                project_decode(layer)

        with scope("wait_a"):
            for tensor in range(3):
                wait_recv(home(layer, tensor).at[0:others], recv_qkv.at[layer, 0, tensor])
        with scope("attend_aa"):
            turn_keys(layer, 0)
            save_cache(layer, 0)
            attend_triangle(layer, 0)
        with scope("wait_q"):
            wait_recv(got_q.at[0:others], recv_qkv.at[layer, 1, 0])
        with scope("attend_ba"):
            attend_square(layer)
        with scope("wait_oa"):
            for tensor in range(3):
                wait_send(sent.at[tensor, 0, 0:others], send_qkv.at[0, tensor])
            wait_recv(mixed_sent.at[0:others], recv_o.at[layer, 0])

        def finish_attention():
            @pl.when(layer > 0)
            def _():
                with scope("project_dec"):
                    project_decode(layer)

            with scope("wait_kv"):
                wait_recv(got.at[layer, pl.ds(0, 2), pl.ds(0, others)], recv_qkv.at[layer, 1, 1])
            wait_send(mixed_sent.at[0:others], send_o.at[0])
            with scope("attend_bb"):
                turn_keys(layer, 1)
                attend_triangle(layer, 1, lambda: attend_decode(layer))
            with scope("attend_dec"):
                save_cache(layer, 1)

        with scope("dense_a"):
            dense(layer, 0, finish_attention)
        with scope("drain_a"):
            wait_send(sent.at[0, 1, 0:others], send_qkv.at[1, 0])
            wait_send(sent.at[pl.ds(1, 2), 1, pl.ds(0, others)], send_qkv.at[1, 1])

        @pl.when(layer < last)
        def _():
            with scope("project_a"):
                normalize_x(0, blk, gain_of(gain_attn, layer + 1))
                project(layer + 1, 0)

        @pl.when(layer == last)
        def _():
            pltpu.make_async_copy(rows_x.at[0:blk], x_out.at[0:blk], sem_out.at[0]).start()

        with scope("wait_ob"):
            wait_recv(mixed_sent.at[0:others], recv_o.at[layer, 1])
            wait_recv(emb_part.at[0:others], recv_d.at[layer])
        with scope("dense_b"):
            dense(layer, 1, None)
        with scope("drain_b"):
            wait_send(mixed_sent.at[0:others], send_o.at[1])
            wait_send(emb_part.at[0:others], send_d)

        @pl.when(layer < last)
        def _():
            normalize_x(blk, b_rows, gain_of(gain_attn, layer + 1))

        return carry

    lax.fori_loop(0, num_layers, layer_body, 0)

    pltpu.make_async_copy(rows_x.at[blk:2 * blk], x_out.at[blk:2 * blk], sem_out.at[1]).start()
    dec_out[...] = rows_x[2 * blk:2 * blk + PAD]
    wait_send(emb_part.at[0:others], send_e)
    wait_send(emb_part.at[0:others], send_f)
    for layer in range(num_layers):
        pltpu.make_async_copy(k_cache.at[layer], k_cache.at[layer], sem_cache.at[layer, 0]).wait()
        pltpu.make_async_copy(v_cache.at[layer], v_cache.at[layer], sem_cache.at[layer, 1]).wait()
    for part in range(2):
        where = pl.ds(part * blk, blk)
        pltpu.make_async_copy(rows_x.at[where], x_out.at[where], sem_out.at[part]).wait()


def place_kernel(x_ref, k_ref, v_ref, dec_ref, x_to, k_to, v_to, dec_to, x_held, k_held, v_held, dec_held, sems):
    moves = ((k_ref, k_held, k_to), (v_ref, v_held, v_to), (x_ref, x_held, x_to))
    for n, (source, held, _) in enumerate(moves):
        pltpu.make_async_copy(source, held, sems.at[0, n]).start()
    pltpu.make_async_copy(dec_ref, dec_held, sems.at[0, 3]).start()
    for n, (source, held, result) in enumerate(moves):
        pltpu.make_async_copy(source, held, sems.at[0, n]).wait()
        pltpu.make_async_copy(held, result, sems.at[1, n]).start()
    pltpu.make_async_copy(dec_ref, dec_held, sems.at[0, 3]).wait()
    dec_to[...] = dec_held[0:dec_to.shape[0]]
    for n, (_, held, result) in enumerate(moves):
        pltpu.make_async_copy(held, result, sems.at[1, n]).wait()


def place(steps, *arrays):
    spec = pl.BlockSpec(memory_space=pl.ANY)
    shapes = [jax.ShapeDtypeStruct(a.shape, a.dtype) for a in arrays]
    shapes[-1] = jax.ShapeDtypeStruct((steps,) + arrays[-1].shape[1:], arrays[-1].dtype)
    return pl.pallas_call(
        place_kernel,
        out_shape=tuple(shapes),
        in_specs=[spec] * len(arrays),
        out_specs=(spec, spec, spec, pl.BlockSpec(memory_space=pltpu.VMEM)),
        scratch_shapes=[pltpu.VMEM(a.shape, a.dtype) for a in arrays] + [pltpu.SemaphoreType.DMA((2, len(arrays)))],
        compiler_params=pltpu.CompilerParams(vmem_limit_bytes=67_000_000),
        name="place",
    )(*arrays)


def solution(mesh):
    group = mesh.shape["cp"]

    def local_program(x_rows, token_ids, table_rows, norm_attn, w_q, w_k, w_v, w_o, norm_mlp, w_gate, w_up, w_down):
        device = lax.axis_index("cp")
        num_layers, d_model, num_heads, head_dim = w_q.shape
        kv_heads = w_k.shape[2]
        ff_dim = w_gate.shape[2]
        seq_dev = x_rows.shape[0]
        blk = seq_dev // 2
        seq_len = group * seq_dev
        steps = token_ids.shape[0]
        heads_dev = num_heads // group
        assert heads_dev * head_dim == LANES and kv_heads == num_heads and blk == LANES

        emb = pick_rows(token_ids, table_rows)

        offsets = jnp.arange(LANES, dtype=jnp.int32)
        positions = jnp.stack([device * blk + offsets, (2 * group - 1 - device) * blk + offsets, seq_len + offsets % head_dim])
        inv_freq = 1.0 / (ROPE_BASE ** (jnp.arange(0, head_dim, 2, dtype=F32) / head_dim))
        angles = positions.astype(F32)[:, None, :] * inv_freq[None, :, None]
        tables = jnp.stack([jnp.cos(angles), jnp.sin(angles)], axis=1).reshape(6, head_dim // 2, LANES)

        def head_rows(w):
            return w.transpose(0, 2, 3, 1).reshape(num_layers * num_heads * head_dim, d_model)

        any_spec = pl.BlockSpec(memory_space=pl.ANY)
        vmem = pl.BlockSpec(memory_space=pltpu.VMEM)
        dma = pltpu.SemaphoreType.DMA
        acc_rows = head_dim + 8
        quarter = KEY_TILE // 2
        tiles = d_model // QKV_ROWS
        pairs = group * blk // KEY_TILE
        scratch = [
            pltpu.VMEM((2 * blk + PAD, d_model), BF16),
            pltpu.VMEM((2 * blk + PAD, d_model), BF16),
            pltpu.VMEM((group, 2 * blk + PAD, LANES), BF16),
            pltpu.VMEM((3, 2, group, LANES, blk), BF16),
            pltpu.VMEM((2 * group, LANES, blk), BF16),
            pltpu.VMEM((num_layers, 2, 2 * group, LANES, blk), BF16),
            pltpu.VMEM((seq_len, LANES), BF16),
            pltpu.VMEM((group, blk, LANES), BF16),
            pltpu.VMEM((2, 2 * heads_dev, KEY_TILE, quarter), F32),
            pltpu.VMEM((2, 2 * heads_dev, 1, quarter), F32),
            pltpu.VMEM((pairs, 2 * heads_dev, 1, quarter), F32),
            pltpu.VMEM((pairs, 2 * heads_dev, acc_rows, quarter), F32),
            pltpu.VMEM((tiles, QKV_ROWS, d_model), BF16),
            pltpu.VMEM((tiles, d_model, QKV_ROWS), BF16),
            pltpu.VMEM((FF_SLOTS, d_model, FF_TILE), BF16),
            pltpu.VMEM((FF_SLOTS, d_model, FF_TILE), BF16),
            pltpu.VMEM((FF_SLOTS, FF_TILE, d_model), BF16),
            pltpu.VMEM((3, LANES, d_model), BF16),
            pltpu.VMEM((LANES, LANES), BF16),
            pltpu.VMEM((LANES, LANES), BF16),
            pltpu.VMEM((LANES, LANES), BF16),
            pltpu.VMEM((blk + PAD, d_model), F32),
            pltpu.VMEM((blk + PAD, FF_TILE), BF16),
            pltpu.VMEM((group, PAD, LANES), BF16),
            pltpu.VMEM((PAD, LANES), BF16),
            pltpu.VMEM((PAD, LANES), BF16),
            dma, dma((tiles,)), dma((tiles,)), dma((3, FF_SLOTS)), dma((3,)),
            dma((2, 3)), dma((num_layers, 2, 3)), dma((2,)), dma((num_layers, 2)), dma, dma((num_layers,)),
            dma, dma, dma, dma, dma((num_layers, 2)), dma((2,)),
        ]
        x_new, k_flat, v_flat, dec = pl.pallas_call(
            functools.partial(main_kernel, group, head_dim, num_layers, steps),
            out_shape=(
                jax.ShapeDtypeStruct((seq_dev, d_model), BF16),
                jax.ShapeDtypeStruct((num_layers, LANES, seq_len), BF16),
                jax.ShapeDtypeStruct((num_layers, LANES, seq_len), BF16),
                jax.ShapeDtypeStruct((PAD, d_model), BF16),
            ),
            in_specs=[any_spec, vmem, vmem, vmem, vmem] + [any_spec] * 7,
            out_specs=(any_spec, any_spec, any_spec, vmem),
            scratch_shapes=scratch,
            compiler_params=pltpu.CompilerParams(collective_id=0, has_side_effects=True, vmem_limit_bytes=67_000_000),
            name="prefill_decode",
        )(
            x_rows, emb, norm_attn, norm_mlp, tables,
            head_rows(w_q), head_rows(w_k), head_rows(w_v), w_o.reshape(num_layers * d_model, d_model),
            w_gate.reshape(num_layers * d_model, ff_dim), w_up.reshape(num_layers * d_model, ff_dim), w_down.reshape(num_layers * ff_dim, d_model),
        )

        def cache(flat):
            return flat.reshape(num_layers, heads_dev, head_dim, seq_len).transpose(0, 3, 1, 2)

        x_new, k_flat, v_flat, dec = place(steps, x_new, k_flat, v_flat, dec)
        return x_new, cache(k_flat), cache(v_flat), dec

    replicated = P()
    in_specs = (P(("req", "cp"), None), P("req"), P("cp", None)) + (replicated,) * 9
    out_specs = (P(("req", "cp"), None), P(None, "req", "cp", None), P(None, "req", "cp", None), P("req", None))
    return jax.shard_map(local_program, mesh=mesh, in_specs=in_specs, out_specs=out_specs, check_vma=False)
```

```python
import functools

import jax
import jax.numpy as jnp
from jax import lax
from jax.experimental import pallas as pl
from jax.experimental.pallas import tpu as pltpu
from jax.sharding import PartitionSpec as P

ROPE_BASE = 10000.0
NORM_EPS = 1e-5
LOG2_E = 1.4426950408889634
BF16 = jnp.bfloat16
F32 = jnp.float32
MESH = pl.DeviceIdType.MESH
LANES = 128
PAD = 16
QKV_ROWS = 512
FF_TILE = 512
FF_SLOTS = 4
KEY_TILE = 512
SPLIT = (14, 12)


def pick_kernel(vocab_dev, ids_ref, table_ref, out_ref, rows, sems):
    steps = ids_ref.shape[0]
    base = lax.axis_index("cp") * vocab_dev

    def copy(t):
        local = jnp.clip(ids_ref[t] - base, 0, vocab_dev - 1)
        start = pl.multiple_of((local // 8) * 8, 8)
        return pltpu.make_async_copy(table_ref.at[pl.ds(start, 8), :], rows.at[t], sems.at[t])

    for t in range(steps):
        copy(t).start()
    out_ref[...] = jnp.zeros_like(out_ref)
    picked = []
    for t in range(steps):
        copy(t).wait()
        local = ids_ref[t] - base
        inside = (local >= 0) & (local < vocab_dev)
        which = jnp.where(inside, lax.rem(jnp.clip(local, 0, vocab_dev - 1), 8), -1)
        index = lax.broadcasted_iota(jnp.int32, rows.shape[1:], 0)
        picked.append(jnp.sum(jnp.where(index == which, rows[t].astype(F32), 0.0), axis=0, keepdims=True))
    picked.append(jnp.zeros((PAD - steps, rows.shape[2]), F32))
    out_ref[...] = jnp.concatenate(picked, axis=0).astype(BF16)


def pick_rows(token_ids, table_rows):
    vocab_dev, d_model = table_rows.shape
    steps = token_ids.shape[0]
    return pl.pallas_call(
        functools.partial(pick_kernel, vocab_dev),
        out_shape=jax.ShapeDtypeStruct((PAD, d_model), BF16),
        in_specs=[
            pl.BlockSpec(memory_space=pltpu.SMEM),
            pl.BlockSpec(memory_space=pl.ANY),
        ],
        out_specs=pl.BlockSpec(memory_space=pltpu.VMEM),
        scratch_shapes=[pltpu.VMEM((steps, 8, d_model), BF16), pltpu.SemaphoreType.DMA((steps,))],
        name="pick_rows",
    )(token_ids, table_rows)


def main_kernel(
    group, head_dim, num_layers, steps,
    x_in, emb_in, gain_attn, gain_mlp, cos_tab, sin_tab, w_q, w_k, w_v, w_o, w_gate, w_up, w_down,
    x_out, k_cache, v_cache, dec_out,
    rows_x, rows_h, mixed, sent, got_q, got, key_rows, mixed_sent, score, best, run_max, run_acc,
    qkv_ring, wo_buf, gate_ring, up_ring, down_ring, dec_w, dec_q, dec_k, dec_v, acc, gated, emb_part, emb_sum, dec_sent,
    sem_x, sem_qkv, sem_wo, sem_ff, sem_dec, send_qkv, recv_qkv, send_o, recv_o, send_d, recv_d, send_e, recv_e, send_f, recv_f, sem_cache, sem_out,
):
    me = lax.axis_index("cp")
    blk = LANES
    blocks = 2 * group
    d_model = rows_x.shape[1]
    ff_dim = w_gate.shape[1]
    ff_steps = ff_dim // FF_TILE
    heads_dev = LANES // head_dim
    per_tile = QKV_ROWS // LANES
    tiles = d_model // QKV_ROWS
    half = head_dim // 2
    pair_blocks = KEY_TILE // blk
    pairs = group // pair_blocks
    exp_scale = float(head_dim ** -0.5 * LOG2_E)
    acc_rows = run_acc.shape[2]
    last = num_layers - 1
    b_rows = blk + PAD
    others = group - 1
    neighbour = lax.rem(me + 1, group)
    w_qkv = (w_q, w_k, w_v)
    order_a = (1, 2, 0)

    def remote(src, dst, ssem, rsem, device):
        return pltpu.make_async_remote_copy(src_ref=src, dst_ref=dst, send_sem=ssem, recv_sem=rsem, device_id={"cp": device}, device_id_type=MESH)

    def wait_recv(ref, sem):
        remote(ref, ref, send_e, sem, neighbour).wait_recv()

    def wait_send(ref, sem):
        remote(ref, ref, sem, recv_e, neighbour).wait_send()

    def tile_of(r):
        return lax.rem(r + me // per_tile + 1, tiles)

    def qkv_copy(layer, tensor, r):
        start = pl.multiple_of(layer * d_model + tile_of(r) * QKV_ROWS, QKV_ROWS)
        return pltpu.make_async_copy(w_qkv[tensor].at[pl.ds(start, QKV_ROWS), :], qkv_ring.at[r], sem_qkv.at[r])

    def wo_copy(layer, n):
        start = pl.multiple_of(layer * d_model, d_model)
        return pltpu.make_async_copy(w_o.at[pl.ds(start, d_model), pl.ds(n * QKV_ROWS, QKV_ROWS)], wo_buf.at[n], sem_wo.at[n])

    def gu_copies(layer, step):
        slot = lax.rem(step, FF_SLOTS)
        start = pl.multiple_of(layer * d_model, d_model)
        col = pl.multiple_of(step * FF_TILE, FF_TILE)
        return (
            pltpu.make_async_copy(w_gate.at[pl.ds(start, d_model), pl.ds(col, FF_TILE)], gate_ring.at[slot], sem_ff.at[0, slot]),
            pltpu.make_async_copy(w_up.at[pl.ds(start, d_model), pl.ds(col, FF_TILE)], up_ring.at[slot], sem_ff.at[1, slot]),
        )

    def down_copy(layer, step):
        slot = lax.rem(step, FF_SLOTS)
        start = pl.multiple_of(layer * ff_dim + step * FF_TILE, FF_TILE)
        return pltpu.make_async_copy(w_down.at[pl.ds(start, FF_TILE), :], down_ring.at[slot], sem_ff.at[2, slot])

    def dec_copy(layer, tensor):
        start = pl.multiple_of(layer * d_model + me * LANES, LANES)
        return pltpu.make_async_copy(w_qkv[tensor].at[pl.ds(start, LANES), :], dec_w.at[tensor], sem_dec.at[tensor])

    def block_of(chunk, device):
        return device if chunk == 0 else blocks - 1 - device

    def home(layer, tensor):
        return got_q if tensor == 0 else got.at[layer, tensor - 1]

    def qkv_piece(layer, tensor, chunk, device):
        return remote(
            sent.at[tensor, chunk, device], home(layer, tensor).at[block_of(chunk, me)],
            send_qkv.at[chunk, tensor], recv_qkv.at[layer, chunk, tensor], device,
        )

    def send_to(piece, device):
        @pl.when(device != me)
        def _():
            piece.start()

    def send_queries(layer):
        def body(i, carry):
            qkv_piece(layer, 0, 1, lax.rem(me + 1 + i, group)).start()
            return carry

        lax.fori_loop(0, others, body, 0)

    def send_rest(layer):
        def body(i, carry):
            device = lax.rem(me + 1 + i, group)
            source, place = sent.at[pl.ds(1, 2), 1, device], got.at[layer, pl.ds(0, 2), block_of(1, me)]
            remote(source, place, send_qkv.at[1, 1], recv_qkv.at[layer, 1, 1], device).start()
            return carry

        lax.fori_loop(0, others, body, 0)

    def gain_of(ref, layer):
        gains = ref[...].astype(F32)
        chosen = gains[0:1]
        for n in range(1, num_layers):
            chosen = jnp.where(layer == n, gains[n:n + 1], chosen)
        return chosen

    def normalize(read, row0, count, gain):
        part = 64 if count % 64 == 0 else 48

        def body(i, carry):
            rows = pl.ds(pl.multiple_of(i * part, 16), part)
            wide = read(rows)
            inv = lax.rsqrt(jnp.mean(wide * wide, axis=-1, keepdims=True) + NORM_EPS)
            rows_h[pl.ds(pl.multiple_of(row0 + i * part, 16), part), :] = (wide * inv * gain).astype(BF16)
            return carry

        lax.fori_loop(0, count // part, body, 0)

    def normalize_x(row0, count, gain):
        def read(rows):
            return rows_x[pl.ds(pl.multiple_of(row0 + rows.start, 16), rows.size), :].astype(F32)

        normalize(read, row0, count, gain)

    def rotate(flat, which):
        cosines, sines = cos_tab[which], sin_tab[which]
        heads = flat.reshape(flat.shape[0] // head_dim, head_dim, flat.shape[1])
        first, second = heads[:, :half], heads[:, half:]
        turned = jnp.concatenate([first * cosines - second * sines, second * cosines + first * sines], axis=1)
        return turned.reshape(flat.shape)

    def project(layer, chunk, between=()):
        order = order_a if chunk == 0 else order_a[::-1]
        for place, tensor in enumerate(order):
            def body(i, carry, place=place, tensor=tensor):
                spots = (2 * i, 2 * i + 1)
                if chunk == 0 or place > 0:
                    for r in spots:
                        qkv_copy(layer, tensor, r).wait()
                for r in spots:
                    flat = lax.dot_general(
                        qkv_ring[r], rows_h[chunk * blk:(chunk + 1) * blk, :], (((1,), (1,)), ((), ())), preferred_element_type=F32
                    )
                    if tensor != 2:
                        flat = rotate(flat, chunk)
                    sent[tensor, chunk, pl.ds(tile_of(r) * per_tile, per_tile)] = flat.astype(BF16).reshape(per_tile, LANES, blk)
                for r in spots:
                    if place < 2:
                        qkv_copy(layer, order[place + 1], r).start()
                    elif chunk == 1:
                        @pl.when(layer < last)
                        def _(r=r):
                            qkv_copy(layer + 1, order_a[0], r).start()
                    if chunk == 0:
                        for k in range(per_tile):
                            device = tile_of(r) * per_tile + k
                            send_to(qkv_piece(layer, tensor, chunk, device), device)
                return carry

            lax.fori_loop(0, tiles // 2, body, 0)
            home(layer, tensor)[block_of(chunk, me)] = sent[tensor, chunk, me]
            if chunk == 1 and tensor == 0:
                send_queries(layer)
            if place < len(between):
                between[place]()

    def project_decode(layer):
        few = rows_h[2 * blk:2 * blk + PAD]
        blank = jnp.zeros((head_dim - PAD, d_model), BF16)
        normed = jnp.concatenate([few, blank] * heads_dev, axis=0)
        for tensor in range(3):
            dec_copy(layer, tensor).wait()
            flat = lax.dot_general(dec_w[tensor], normed, (((1,), (1,)), ((), ())), preferred_element_type=F32)
            if tensor != 2:
                flat = rotate(flat, 2)
            if tensor == 0:
                row = lax.broadcasted_iota(jnp.int32, flat.shape, 0) // head_dim
                col = lax.broadcasted_iota(jnp.int32, flat.shape, 1) // head_dim
                dec_q[...] = jnp.where(row == col, flat, 0.0).astype(BF16)
            elif tensor == 1:
                dec_k[...] = flat.T.astype(BF16)
            else:
                dec_v[...] = flat.astype(BF16)

        @pl.when(layer < last)
        def _():
            for tensor in range(3):
                dec_copy(layer + 1, tensor).start()

    def turn_keys(layer, chunk):
        def body(i, carry):
            for u in range(4):
                j = chunk * group + 4 * i + u
                key_rows[pl.ds(pl.multiple_of(j * blk, blk), blk), :] = got[layer, 0, j].astype(F32).T.astype(BF16)
            return carry

        lax.fori_loop(0, group // 4, body, 0)

    def save_cache(layer, chunk):
        def body(i, carry):
            j = chunk * group + i
            place = pl.ds(pl.multiple_of(j * blk, blk), blk)
            pltpu.make_async_copy(got.at[layer, 0, j], k_cache.at[layer, :, place], sem_cache.at[layer, 0]).start()
            pltpu.make_async_copy(got.at[layer, 1, j], v_cache.at[layer, :, place], sem_cache.at[layer, 1]).start()
            return carry

        lax.fori_loop(0, group, body, 0)

    def scores(layer, pair, tile, slot):
        keys = key_rows[pl.ds(pl.multiple_of(tile * KEY_TILE, KEY_TILE), KEY_TILE), :]
        for u in range(2):
            query = jnp.concatenate([got_q[pair_blocks * pair + 2 * u], got_q[pair_blocks * pair + 2 * u + 1]], axis=1)
            blank = jnp.zeros((head_dim, query.shape[1]), BF16)
            for h in range(heads_dev):
                parts = [blank] * heads_dev
                parts[h] = query[h * head_dim:(h + 1) * head_dim]
                value = jnp.dot(keys, jnp.concatenate(parts, axis=0), preferred_element_type=F32)
                score[slot, 2 * u + h] = value
                best[slot, 2 * u + h] = jnp.max(value, axis=0, keepdims=True)

    def absorb(layer, tile, slot, place, diagonal=False, first=False):
        held = [got[layer, 1, tile * pair_blocks + i] for i in range(pair_blocks)]
        for u in range(2):
            count = pair_blocks // 2 if diagonal and u == 0 else pair_blocks
            ones = jnp.ones((acc_rows - head_dim, count * blk), BF16)
            for h in range(heads_dev):
                c = 2 * u + h
                new = best[slot, c] if first else jnp.maximum(run_max[place, c], best[slot, c])
                probs = jnp.exp2((score[slot, c, :count * blk] - new) * exp_scale).astype(BF16)
                value = jnp.concatenate([jnp.concatenate([b[h * head_dim:(h + 1) * head_dim] for b in held[:count]], axis=1), ones], axis=0)
                added = jnp.dot(value, probs, preferred_element_type=F32)
                if first:
                    run_acc[place, c] = added
                else:
                    run_acc[place, c] = run_acc[place, c] * jnp.exp2((run_max[place, c] - new) * exp_scale) + added
                run_max[place, c] = new

    def mask_diagonal(slot):
        width = score.shape[3]
        key = lax.broadcasted_iota(jnp.int32, (width, width), 0)
        query = lax.broadcasted_iota(jnp.int32, (width, width), 1)
        for u in range(2):
            rows = slice(u * width, (u + 1) * width)
            for h in range(heads_dev):
                c = 2 * u + h
                value = jnp.where(key <= query, score[slot, c, rows], -jnp.inf)
                score[slot, c, rows] = value
                top = jnp.max(value, axis=0, keepdims=True)
                if u == 1:
                    top = jnp.maximum(top, jnp.max(score[slot, c, :width], axis=0, keepdims=True))
                best[slot, c] = top

    def turn_out(place):
        for u in range(2):
            full = jnp.concatenate(
                [run_acc[place, 2 * u + h, :head_dim] / run_acc[place, 2 * u + h, head_dim:head_dim + 1] for h in range(heads_dev)], axis=0
            )
            turned = full.T.astype(BF16)
            for i in range(2):
                mixed_sent[pair_blocks * place + 2 * u + i] = turned[i * blk:(i + 1) * blk]

    def hand_out(layer, chunk, place):
        for i in range(pair_blocks):
            j = pair_blocks * place + i
            device = j if chunk == 0 else group - 1 - j
            where = mixed.at[me, chunk * blk:(chunk + 1) * blk]
            send_to(remote(mixed_sent.at[j], where, send_o.at[chunk], recv_o.at[layer, chunk], device), device)

            @pl.when(device == me)
            def _(j=j):
                mixed[me, chunk * blk:(chunk + 1) * blk] = mixed_sent[j]

    def attend_triangle(layer, chunk, middle=None):
        base = chunk * pairs
        quarter = me // (group // pairs)
        turn = lax.rem(quarter + 1 if chunk == 0 else pairs - quarter, pairs)
        first_slot = [0]
        for pair in range(pairs - 1):
            first_slot.append((first_slot[-1] + pair + 1) % 2)

        def one_pair(pair, i):
            slot = first_slot[pair]
            then = jnp.where(i == pairs - 1, pair, (pair + 1) % pairs)
            for tile in range(pair + 1):
                after = (pair, tile + 1) if tile < pair else (then, 0)
                scores(layer, base + after[0], base + after[1], 1 - slot)
                if tile == pair:
                    mask_diagonal(slot)
                absorb(layer, base + tile, slot, pair, diagonal=tile == pair, first=tile == 0 and chunk == 0)
                slot = 1 - slot
            turn_out(pair)
            hand_out(layer, chunk, pair)

        for pair in range(pairs):
            @pl.when(turn == pair)
            def _(pair=pair):
                scores(layer, base + pair, base, first_slot[pair])

        def body(i, carry):
            for pair in range(pairs):
                @pl.when(lax.rem(turn + i, pairs) == pair)
                def _(pair=pair):
                    one_pair(pair, i)
            if middle is not None:
                pl.when(i == pairs // 2 - 1)(middle)
            return carry

        lax.fori_loop(0, pairs, body, 0)

    def attend_square(layer):
        scores(layer, pairs, 0, 0)

        def body(pair, carry):
            for tile in range(pairs):
                if tile + 1 < pairs:
                    scores(layer, pairs + pair, tile + 1, (tile + 1) % 2)
                else:
                    scores(layer, pairs + jnp.minimum(pair + 1, pairs - 1), 0, 0)
                absorb(layer, tile, tile % 2, pair, first=tile == 0)

            @pl.when(pair == jnp.where(layer == 0, pairs - 1, pairs - 2))
            def _():
                send_rest(layer)

            return carry

        lax.fori_loop(0, pairs, body, 0)

    def attend_decode(layer):
        ones = jnp.ones((PAD, KEY_TILE), BF16)
        queries = dec_q[...]
        value = jnp.dot(dec_k[...], queries, preferred_element_type=F32)
        key = lax.broadcasted_iota(jnp.int32, value.shape, 0)
        query = lax.rem(lax.broadcasted_iota(jnp.int32, value.shape, 1), head_dim)
        value = jnp.where((key <= query) & (key < steps), value, -jnp.inf)
        top = jnp.max(value, axis=0, keepdims=True)

        def old(tile):
            return jnp.dot(key_rows[tile * KEY_TILE:(tile + 1) * KEY_TILE, :], queries, preferred_element_type=F32)

        for tile in range(blocks // pair_blocks):
            top = jnp.maximum(top, jnp.max(old(tile), axis=0, keepdims=True))
        held = jnp.concatenate([dec_v[...], ones[:, :LANES]], axis=0)
        total = jnp.dot(held, jnp.exp2((value - top) * exp_scale).astype(BF16), preferred_element_type=F32)
        for tile in range(blocks // pair_blocks):
            held = jnp.concatenate([got[layer, 1, tile * pair_blocks + k] for k in range(pair_blocks)], axis=1)
            probs = jnp.exp2((old(tile) - top) * exp_scale).astype(BF16)
            total = total + jnp.dot(jnp.concatenate([held, ones], axis=0), probs, preferred_element_type=F32)
        turned = (total[:LANES] / total[LANES:LANES + 1]).T
        lane = lax.broadcasted_iota(jnp.int32, (PAD, LANES), 1)
        result = turned[0:PAD]
        for h in range(1, heads_dev):
            result = jnp.where(lane >= h * head_dim, turned[h * head_dim:h * head_dim + PAD], result)
        dec_sent[...] = result.astype(BF16)
        mixed[me, 2 * blk:2 * blk + PAD] = dec_sent[...]

        def send(i, carry):
            device = lax.rem(me + 1 + i, group)
            remote(dec_sent, mixed.at[me, 2 * blk:2 * blk + PAD], send_d, recv_d.at[layer], device).start()
            return carry

        lax.fori_loop(0, others, send, 0)

    def dense(layer, chunk, between):
        row0, count = (0, blk) if chunk == 0 else (blk, b_rows)
        rows = slice(row0, row0 + count)
        heads = jnp.concatenate([mixed[n, rows] for n in range(group)], axis=1)
        for n in range(tiles):
            if chunk == 0:
                wo_copy(layer, n).wait()
            cols = slice(n * QKV_ROWS, (n + 1) * QKV_ROWS)
            added = rows_x[rows, cols].astype(F32) + jnp.dot(heads, wo_buf[n], preferred_element_type=F32)
            acc[:count, cols] = added.astype(BF16).astype(F32)
        normalize(lambda r: acc[r, :], row0, count, gain_of(gain_mlp, layer))

        def step_at(k):
            return k if chunk == 0 else ff_steps - 1 - k

        def widen(k):
            step = step_at(k)
            slot = lax.rem(step, FF_SLOTS)

            def ready():
                for copy in gu_copies(layer, step):
                    copy.wait()

            if chunk == 0:
                ready()
            else:
                pl.when(k >= FF_SLOTS)(ready)
            normed = rows_h[rows, :]
            gate = jnp.dot(normed, gate_ring[slot], preferred_element_type=F32)
            upward = jnp.dot(normed, up_ring[slot], preferred_element_type=F32)
            gated[:count] = (jax.nn.silu(gate) * upward).astype(BF16)

        def narrow(k):
            step = step_at(k)
            slot = lax.rem(step, FF_SLOTS)

            def ready():
                down_copy(layer, step).wait()

            if chunk == 0:
                ready()
            else:
                pl.when(k >= FF_SLOTS)(ready)
            acc[:count] += jnp.dot(gated[:count], down_ring[slot], preferred_element_type=F32)

        def refill(k, start):
            if chunk == 0:
                @pl.when(k + FF_SLOTS < ff_steps)
                def _():
                    start(layer, k + FF_SLOTS)
            else:
                step = step_at(k)

                @pl.when(step >= FF_SLOTS)
                def _():
                    start(layer, step - FF_SLOTS)

        def start_gu(which, step):
            for copy in gu_copies(which, step):
                copy.start()

        def start_down(which, step):
            down_copy(which, step).start()

        widen(0)
        refill(0, start_gu)

        def body(k, carry):
            narrow(k - 1)
            widen(k)
            refill(k - 1, start_down)
            refill(k, start_gu)
            return carry

        if between is None:
            lax.fori_loop(1, ff_steps, body, 0)
        else:
            split = jnp.where(layer == 0, SPLIT[0], SPLIT[1])
            lax.fori_loop(1, split, body, 0)
            between()
            lax.fori_loop(split, ff_steps, body, 0)
        narrow(ff_steps - 1)
        refill(ff_steps - 1, start_down)
        rows_x[rows, :] = acc[:count].astype(BF16)

    scope = jax.named_scope
    pltpu.make_async_copy(x_in, rows_x.at[0:2 * blk], sem_x).start()
    barrier = pltpu.get_barrier_semaphore()
    for i in range(1, group):
        pl.semaphore_signal(barrier, inc=1, device_id={"cp": lax.rem(me + i, group)}, device_id_type=MESH)
    qkv_copy(0, order_a[0], 0).start()
    pltpu.make_async_copy(x_in, rows_x.at[0:2 * blk], sem_x).wait()
    for r in range(1, tiles):
        qkv_copy(0, order_a[0], r).start()
    for tensor in range(3):
        dec_copy(0, tensor).start()
    with scope("norm_first"):
        normalize_x(0, blk, gain_of(gain_attn, 0))
    with scope("barrier"):
        pl.semaphore_wait(barrier, others)

    my_cols = pl.ds(pl.multiple_of(me * LANES, LANES), LANES)

    def split_looked_up():
        def part_out(i, carry):
            device = lax.rem(me + 1 + i, group)
            cols = pl.ds(pl.multiple_of(device * LANES, LANES), LANES)
            remote(emb_in.at[:, cols], emb_part.at[me], send_e, recv_e, device).start()
            return carry

        lax.fori_loop(0, others, part_out, 0)
        emb_part[me] = emb_in[:, my_cols]

    def sum_looked_up():
        with scope("embed"):
            wait_recv(emb_part.at[0:others], recv_e)
            emb_sum[...] = jnp.sum(emb_part[...].astype(F32), axis=0).astype(BF16)
            rows_x[2 * blk:2 * blk + PAD, my_cols] = emb_sum[...]

            def sum_out(i, carry):
                device = lax.rem(me + 1 + i, group)
                remote(emb_sum, rows_x.at[2 * blk:2 * blk + PAD, my_cols], send_f, recv_f, device).start()
                return carry

            lax.fori_loop(0, others, sum_out, 0)

    with scope("project_first"):
        project(0, 0, (split_looked_up, sum_looked_up))
        normalize_x(blk, blk, gain_of(gain_attn, 0))

    def layer_body(layer, carry):
        with scope("project_b"):
            project(layer, 1)

        for n in range(tiles):
            wo_copy(layer, n).start()
        for step in range(FF_SLOTS):
            for copy in gu_copies(layer, step):
                copy.start()
            down_copy(layer, step).start()

        @pl.when(layer == 0)
        def _():
            wait_recv(emb_part.at[0:others], recv_f)
            wide = rows_x[2 * blk:2 * blk + PAD].astype(F32)
            inv = lax.rsqrt(jnp.mean(wide * wide, axis=-1, keepdims=True) + NORM_EPS)
            rows_h[2 * blk:2 * blk + PAD] = (wide * inv * gain_of(gain_attn, 0)).astype(BF16)
            with scope("project_dec"):
                project_decode(layer)

        with scope("wait_a"):
            for tensor in range(3):
                wait_recv(home(layer, tensor).at[0:others], recv_qkv.at[layer, 0, tensor])
        with scope("attend_aa"):
            turn_keys(layer, 0)
            save_cache(layer, 0)
            attend_triangle(layer, 0)
        with scope("wait_q"):
            wait_recv(got_q.at[0:others], recv_qkv.at[layer, 1, 0])
        with scope("attend_ba"):
            attend_square(layer)
        with scope("wait_oa"):
            for tensor in range(3):
                wait_send(sent.at[tensor, 0, 0:others], send_qkv.at[0, tensor])
            wait_recv(mixed_sent.at[0:others], recv_o.at[layer, 0])

        def finish_attention():
            @pl.when(layer > 0)
            def _():
                with scope("project_dec"):
                    project_decode(layer)

            with scope("wait_kv"):
                wait_recv(got.at[layer, pl.ds(0, 2), pl.ds(0, others)], recv_qkv.at[layer, 1, 1])
            wait_send(mixed_sent.at[0:others], send_o.at[0])
            with scope("attend_bb"):
                turn_keys(layer, 1)
                attend_triangle(layer, 1, lambda: attend_decode(layer))
            with scope("attend_dec"):
                save_cache(layer, 1)

        with scope("dense_a"):
            dense(layer, 0, finish_attention)
        with scope("drain_a"):
            wait_send(sent.at[0, 1, 0:others], send_qkv.at[1, 0])
            wait_send(sent.at[pl.ds(1, 2), 1, pl.ds(0, others)], send_qkv.at[1, 1])

        @pl.when(layer < last)
        def _():
            with scope("project_a"):
                normalize_x(0, blk, gain_of(gain_attn, layer + 1))
                project(layer + 1, 0)

        @pl.when(layer == last)
        def _():
            pltpu.make_async_copy(rows_x.at[0:blk], x_out.at[0:blk], sem_out.at[0]).start()

        with scope("wait_ob"):
            wait_recv(mixed_sent.at[0:others], recv_o.at[layer, 1])
            wait_recv(emb_part.at[0:others], recv_d.at[layer])
        with scope("dense_b"):
            dense(layer, 1, None)
        with scope("drain_b"):
            wait_send(mixed_sent.at[0:others], send_o.at[1])
            wait_send(emb_part.at[0:others], send_d)

        @pl.when(layer < last)
        def _():
            normalize_x(blk, b_rows, gain_of(gain_attn, layer + 1))

        return carry

    lax.fori_loop(0, num_layers, layer_body, 0)

    pltpu.make_async_copy(rows_x.at[blk:2 * blk], x_out.at[blk:2 * blk], sem_out.at[1]).start()
    dec_out[...] = rows_x[2 * blk:2 * blk + PAD]
    wait_send(emb_part.at[0:others], send_e)
    wait_send(emb_part.at[0:others], send_f)
    for layer in range(num_layers):
        pltpu.make_async_copy(k_cache.at[layer], k_cache.at[layer], sem_cache.at[layer, 0]).wait()
        pltpu.make_async_copy(v_cache.at[layer], v_cache.at[layer], sem_cache.at[layer, 1]).wait()
    for part in range(2):
        where = pl.ds(part * blk, blk)
        pltpu.make_async_copy(rows_x.at[where], x_out.at[where], sem_out.at[part]).wait()


def place_kernel(x_ref, k_ref, v_ref, dec_ref, x_to, k_to, v_to, dec_to, x_held, k_held, v_held, dec_held, sems):
    moves = ((k_ref, k_held, k_to), (v_ref, v_held, v_to), (x_ref, x_held, x_to))
    for n, (source, held, _) in enumerate(moves):
        pltpu.make_async_copy(source, held, sems.at[0, n]).start()
    pltpu.make_async_copy(dec_ref, dec_held, sems.at[0, 3]).start()
    for n, (source, held, result) in enumerate(moves):
        pltpu.make_async_copy(source, held, sems.at[0, n]).wait()
        pltpu.make_async_copy(held, result, sems.at[1, n]).start()
    pltpu.make_async_copy(dec_ref, dec_held, sems.at[0, 3]).wait()
    dec_to[...] = dec_held[0:dec_to.shape[0]]
    for n, (_, held, result) in enumerate(moves):
        pltpu.make_async_copy(held, result, sems.at[1, n]).wait()


def place(steps, *arrays):
    spec = pl.BlockSpec(memory_space=pl.ANY)
    shapes = [jax.ShapeDtypeStruct(a.shape, a.dtype) for a in arrays]
    shapes[-1] = jax.ShapeDtypeStruct((steps,) + arrays[-1].shape[1:], arrays[-1].dtype)
    return pl.pallas_call(
        place_kernel,
        out_shape=tuple(shapes),
        in_specs=[spec] * len(arrays),
        out_specs=(spec, spec, spec, pl.BlockSpec(memory_space=pltpu.VMEM)),
        scratch_shapes=[pltpu.VMEM(a.shape, a.dtype) for a in arrays] + [pltpu.SemaphoreType.DMA((2, len(arrays)))],
        compiler_params=pltpu.CompilerParams(vmem_limit_bytes=67_000_000),
        name="place",
    )(*arrays)


def solution(mesh):
    group = mesh.shape["cp"]

    def local_program(x_rows, token_ids, table_rows, norm_attn, w_q, w_k, w_v, w_o, norm_mlp, w_gate, w_up, w_down):
        device = lax.axis_index("cp")
        num_layers, d_model, num_heads, head_dim = w_q.shape
        kv_heads = w_k.shape[2]
        ff_dim = w_gate.shape[2]
        seq_dev = x_rows.shape[0]
        blk = seq_dev // 2
        seq_len = group * seq_dev
        steps = token_ids.shape[0]
        heads_dev = num_heads // group
        assert heads_dev * head_dim == LANES and kv_heads == num_heads and blk == LANES

        emb = pick_rows(token_ids, table_rows)

        offsets = jnp.arange(LANES, dtype=jnp.int32)
        positions = jnp.stack([device * blk + offsets, (2 * group - 1 - device) * blk + offsets, seq_len + offsets % head_dim])
        inv_freq = 1.0 / (ROPE_BASE ** (jnp.arange(0, head_dim, 2, dtype=F32) / head_dim))
        angles = positions.astype(F32)[:, None, :] * inv_freq[None, :, None]
        def head_rows(w):
            return w.transpose(0, 2, 3, 1).reshape(num_layers * num_heads * head_dim, d_model)

        any_spec = pl.BlockSpec(memory_space=pl.ANY)
        vmem = pl.BlockSpec(memory_space=pltpu.VMEM)
        dma = pltpu.SemaphoreType.DMA
        acc_rows = head_dim + 8
        quarter = KEY_TILE // 2
        tiles = d_model // QKV_ROWS
        pairs = group * blk // KEY_TILE
        scratch = [
            pltpu.VMEM((2 * blk + PAD, d_model), BF16),
            pltpu.VMEM((2 * blk + PAD, d_model), BF16),
            pltpu.VMEM((group, 2 * blk + PAD, LANES), BF16),
            pltpu.VMEM((3, 2, group, LANES, blk), BF16),
            pltpu.VMEM((2 * group, LANES, blk), BF16),
            pltpu.VMEM((num_layers, 2, 2 * group, LANES, blk), BF16),
            pltpu.VMEM((seq_len, LANES), BF16),
            pltpu.VMEM((group, blk, LANES), BF16),
            pltpu.VMEM((2, 2 * heads_dev, KEY_TILE, quarter), F32),
            pltpu.VMEM((2, 2 * heads_dev, 1, quarter), F32),
            pltpu.VMEM((pairs, 2 * heads_dev, 1, quarter), F32),
            pltpu.VMEM((pairs, 2 * heads_dev, acc_rows, quarter), F32),
            pltpu.VMEM((tiles, QKV_ROWS, d_model), BF16),
            pltpu.VMEM((tiles, d_model, QKV_ROWS), BF16),
            pltpu.VMEM((FF_SLOTS, d_model, FF_TILE), BF16),
            pltpu.VMEM((FF_SLOTS, d_model, FF_TILE), BF16),
            pltpu.VMEM((FF_SLOTS, FF_TILE, d_model), BF16),
            pltpu.VMEM((3, LANES, d_model), BF16),
            pltpu.VMEM((LANES, LANES), BF16),
            pltpu.VMEM((LANES, LANES), BF16),
            pltpu.VMEM((LANES, LANES), BF16),
            pltpu.VMEM((blk + PAD, d_model), F32),
            pltpu.VMEM((blk + PAD, FF_TILE), BF16),
            pltpu.VMEM((group, PAD, LANES), BF16),
            pltpu.VMEM((PAD, LANES), BF16),
            pltpu.VMEM((PAD, LANES), BF16),
            dma, dma((tiles,)), dma((tiles,)), dma((3, FF_SLOTS)), dma((3,)),
            dma((2, 3)), dma((num_layers, 2, 3)), dma((2,)), dma((num_layers, 2)), dma, dma((num_layers,)),
            dma, dma, dma, dma, dma((num_layers, 2)), dma((2,)),
        ]
        x_new, k_flat, v_flat, dec = pl.pallas_call(
            functools.partial(main_kernel, group, head_dim, num_layers, steps),
            out_shape=(
                jax.ShapeDtypeStruct((seq_dev, d_model), BF16),
                jax.ShapeDtypeStruct((num_layers, LANES, seq_len), BF16),
                jax.ShapeDtypeStruct((num_layers, LANES, seq_len), BF16),
                jax.ShapeDtypeStruct((PAD, d_model), BF16),
            ),
            in_specs=[any_spec] + [vmem] * 5 + [any_spec] * 7,
            out_specs=(any_spec, any_spec, any_spec, vmem),
            scratch_shapes=scratch,
            compiler_params=pltpu.CompilerParams(collective_id=0, has_side_effects=True, vmem_limit_bytes=67_000_000),
            name="prefill_decode",
        )(
            x_rows, emb, norm_attn, norm_mlp, jnp.cos(angles), jnp.sin(angles),
            head_rows(w_q), head_rows(w_k), head_rows(w_v), w_o.reshape(num_layers * d_model, d_model),
            w_gate.reshape(num_layers * d_model, ff_dim), w_up.reshape(num_layers * d_model, ff_dim), w_down.reshape(num_layers * ff_dim, d_model),
        )

        def cache(flat):
            return flat.reshape(num_layers, heads_dev, head_dim, seq_len).transpose(0, 3, 1, 2)

        x_new, k_flat, v_flat, dec = place(steps, x_new, k_flat, v_flat, dec)
        return x_new, cache(k_flat), cache(v_flat), dec

    replicated = P()
    in_specs = (P(("req", "cp"), None), P("req"), P("cp", None)) + (replicated,) * 9
    out_specs = (P(("req", "cp"), None), P(None, "req", "cp", None), P(None, "req", "cp", None), P("req", None))
    return jax.shard_map(local_program, mesh=mesh, in_specs=in_specs, out_specs=out_specs, check_vma=False)
```
